32 devices in a mesh: tm: 8 (over y, x, core), space: 4 (over z).
Axes of the slice: x: 2, y: 2, z: 4, core: 2. Of those that a mesh axis runs over, the one named last changes fastest.
Arguments:
- rhs: float32 [16, 1024, 1024], P('tm', 'space'), may hold values from -6 to 6
- guess: float32 [16, 1024, 1024], P('tm', 'space'), may hold values from -6 to 6
- diffusion: float32 [1024, 1024], P('space'), may hold values from 0.2 to 2
Outputs:
- solution: float32 [16, 1024, 1024], P('tm', 'space')
- norms: float32 [6], replicated
The draws below stay inside these ranges and needn't reach their ends.
All inputs are finite; a program needn't handle non-finite values.
Results may differ from the reference program's by a relative error of at most 0.0001.
Values sent between devices are 32-bit elements; how exact they have to be, the bound alone decides.
A program may use at most 64 MiB of HBM per device.

```python
import math
import jax
import jax.numpy as jnp

NY = 1024
LEVELS = 5
NT = 16
NX = 1024


def levels(own_key, extent, split, smallest, high):
    loudness = 1.0
    for dim, shards_of in split:
        steps = jax.random.uniform(jax.random.fold_in(jax.random.fold_in(own_key, 6), dim), (shards_of,), jnp.float32, smallest / len(split), high / len(split))
        loudness = loudness * jnp.repeat(jnp.exp(steps), extent[dim] // shards_of).reshape((-1,) + (1,) * (len(extent) - 1 - dim))
    return loudness


def centred(rng, dims, spread, limit, pieces=(), held_as=jnp.bfloat16):
    gain = levels(rng, dims, pieces, -0.22, 0.18) if pieces else 1.0
    values = jax.random.normal(rng, dims, jnp.float32) * spread * gain
    return jnp.minimum(jnp.maximum(values, -limit), limit).astype(held_as)


def setup_inputs(seed: int = 0) -> dict:
    streams_of = jax.random.split(jax.random.key(seed), 4)
    rhs = centred(streams_of[0], (NT, NX, NY), 1.0, 6.0, ((0, 8), (1, 4)), jnp.float32)
    guess = centred(streams_of[1], (NT, NX, NY), 1.0, 6.0, ((0, 8), (1, 4)), jnp.float32)
    diffusion = jnp.clip(jnp.exp(math.log(2.0) - 2.3025851 * jax.random.uniform(streams_of[2], (NX, NY), jnp.float32) ** levels(streams_of[2], (NX, NY), ((0, 4),), -0.2, 0.2)), 0.2, 2.0)
    return dict(rhs=rhs, guess=guess, diffusion=diffusion)


def neighbours(field):
    padded = jnp.pad(field, ((0, 0), (1, 1), (1, 1)))
    total = padded[:, 2:, 1:-1] + padded[:, :-2, 1:-1]
    total = total + padded[:, 1:-1, 2:] + padded[:, 1:-1, :-2]
    return total

def residual(field, source, scaled, diag):
    before = jnp.concatenate([jnp.zeros_like(field[:1]), field[:-1]], axis=0)
    image = diag * field - scaled * neighbours(field) - before
    return source - image

def reference(rhs, guess, diffusion):
    damping = 0.8
    cells = rhs.shape[1] * rhs.shape[2]
    squares = []
    sources = [rhs]
    fields = []
    field = guess
    for level in range(LEVELS - 1):
        source = sources[level]
        scaled = 2.0 ** level * diffusion
        diag = 1.0 + 4.0 * scaled
        if level == 0:
            field = field + damping * residual(field, source, scaled, diag) / diag
        else:
            field = damping * source / diag
        resid = residual(field, source, scaled, diag)
        squares.append(jnp.sum(resid * resid))
        fields.append(field)
        sources.append(resid[0::2] + resid[1::2])
    level = LEVELS - 1
    source = sources[level]
    scaled = 2.0 ** level * diffusion
    diag = 1.0 + 4.0 * scaled
    field = damping * source / diag
    field = field + damping * residual(field, source, scaled, diag) / diag
    resid = residual(field, source, scaled, diag)
    squares.append(jnp.sum(resid * resid))
    correction = field
    for level in range(LEVELS - 2, -1, -1):
        scaled = 2.0 ** level * diffusion
        diag = 1.0 + 4.0 * scaled
        field = fields[level] + jnp.repeat(correction, 2, axis=0)
        field = field + damping * residual(field, sources[level], scaled, diag) / diag
        correction = field
    scaled = 1.0 * diffusion
    diag = 1.0 + 4.0 * scaled
    resid = residual(correction, rhs, scaled, diag)
    squares.append(jnp.sum(resid * resid))
    norms = jnp.sqrt(jnp.stack(squares) / cells)
    return (correction, norms)
```

```python
import functools

import jax
import jax.numpy as jnp
from jax import lax
from jax.experimental import pallas as pl
from jax.experimental.pallas import tpu as pltpu
from jax.sharding import PartitionSpec as P

LEVELS = 5


damping = 0.8


def with_halo(block, sides, width):
    for axis, dim in sides:
        count = lax.axis_size(axis)
        forward = [(i, i + 1) for i in range(count - 1)]
        backward = [(target, source) for source, target in forward]
        low = lax.ppermute(
            lax.slice_in_dim(block, block.shape[dim] - width, None, axis=dim), axis, forward
        )
        high = lax.ppermute(lax.slice_in_dim(block, 0, width, axis=dim), axis, backward)
        block = jnp.concatenate([low, block, high], axis=dim)
    return block


def shifted(value, axis, steps):
    count = lax.axis_size(axis)
    first, last = (max(0, -steps), min(count, count - steps))
    return lax.ppermute(value, axis, [(source, source + steps) for source in range(first, last)])


def from_partner(value, axis, apart):
    mask = 2**apart
    pairs = [(source, source ^ mask) for source in range(lax.axis_size(axis))]
    return lax.ppermute(value, axis, pairs)


def neighbours(field):
    rows = with_halo(field, (("space", 1),), 1)
    padded = jnp.pad(rows, ((0, 0), (0, 0), (1, 1)))
    total = padded[:, 2:, 1:-1] + padded[:, :-2, 1:-1]
    total = total + padded[:, 1:-1, 2:] + padded[:, 1:-1, :-2]
    return total


def residual(field, source, scaled, diag, stride):
    earlier = shifted(field[-1:], "tm", stride)
    before = jnp.concatenate([earlier, field[:-1]], axis=0)
    image = diag * field - scaled * neighbours(field) - before
    return source - image


def stride_of(level):
    if level == 0:
        return 1
    return 2 ** (level - 1)


def body(rhs, guess, diffusion):
    position = lax.axis_index("tm")
    cells = rhs.shape[1] * lax.axis_size("space") * rhs.shape[2]
    partials = []

    def weight_of(level):
        if level <= 1:
            return jnp.float32(1.0)
        stride = stride_of(level)
        return jnp.where(position % stride == stride - 1, 1.0, 0.0).astype(jnp.float32)

    def record(resid, level):
        local_part = jnp.sum(resid * resid) * weight_of(level)
        partials.append(local_part)

    sources = [rhs]
    fields = []
    field = guess
    for level in range(LEVELS - 1):
        source = sources[level]
        scaled = 2.0**level * diffusion
        diag = 1.0 + 4.0 * scaled
        stride = stride_of(level)
        if level == 0:
            field = field + damping * residual(field, source, scaled, diag, stride) / diag
        else:
            field = damping * source / diag
        resid = residual(field, source, scaled, diag, stride)
        record(resid, level)
        fields.append(field)
        if level == 0:
            coarse = resid[0:1] + resid[1:2]
        else:
            coarse = resid + from_partner(resid, "tm", level - 1)
        sources.append(coarse)
    level = LEVELS - 1
    source = sources[level]
    scaled = 2.0**level * diffusion
    diag = 1.0 + 4.0 * scaled
    stride = stride_of(level)
    field = damping * source / diag
    field = field + damping * residual(field, source, scaled, diag, stride) / diag
    resid = residual(field, source, scaled, diag, stride)
    record(resid, level)
    correction = field
    for level in range(LEVELS - 2, -1, -1):
        scaled = 2.0**level * diffusion
        diag = 1.0 + 4.0 * scaled
        stride = stride_of(level)
        field = fields[level] + correction
        field = field + damping * residual(field, sources[level], scaled, diag, stride) / diag
        correction = field
    scaled = 1.0 * diffusion
    diag = 1.0 + 4.0 * scaled
    resid = residual(correction, rhs, scaled, diag, 1)
    record(resid, 0)
    totals = lax.psum(jnp.stack(partials), ("tm", "space"))
    norms = jnp.sqrt(totals / cells)
    return (correction, norms)


DEVICE = pl.DeviceIdType.MESH
TILE = 8
EDGE = 2 * TILE
BLOCK = 32


def cycle_kernel(
    strips, devices, cells,
    rhs_in, guess_in, diff_in, out, norms_out,
    rhs, guess, diff, v0, g1, v1f, sol, guess_e, v0_e, v1f_e, early, early_e, weights,
    c_weights, c_sources, c_fields, c_finals, tile, gathered, gathered_z,
    load_sem, store_sem, zs_sem, zr_sem, ts_sem, tr_sem, as_sem, ar_sem, al_sem,
    bs_sem, br_sem, bl_sem, rs_sem, ns_sem, nr_sem, ms_sem, mr_sem,
):
    me = lax.axis_index("tm")
    strip = lax.axis_index("space")
    rows, width = rhs_in.shape[1], rhs_in.shape[2]
    core = lax.rem(me, 2)
    sibling = me + 1 - 2 * core
    low, high = EDGE, EDGE + rows
    first, last = me == 0, me == devices - 1
    top, bottom = strip == 0, strip == strips - 1
    piece = rows // devices
    tall_piece = piece + 2 * TILE

    def aligned(value):
        return pl.multiple_of(value, TILE)

    def tm_copy(src, dst, send, recv, target):
        return pltpu.make_async_remote_copy(
            src_ref=src, dst_ref=dst, send_sem=send, recv_sem=recv,
            device_id={"tm": target, "space": strip}, device_id_type=DEVICE,
        )

    def space_copy(src, dst, send, recv, target):
        return pltpu.make_async_remote_copy(
            src_ref=src, dst_ref=dst, send_sem=send, recv_sem=recv,
            device_id={"tm": me, "space": target}, device_id_type=DEVICE,
        )

    later = jnp.minimum(me + 1, devices - 1)
    loads = [
        pltpu.make_async_copy(guess_in, guess.at[:, low:high], load_sem.at[0]),
        pltpu.make_async_copy(diff_in, diff.at[low:high], load_sem.at[1]),
        pltpu.make_async_copy(rhs_in, rhs.at[:, low:high], load_sem.at[2]),
    ]
    for copy in loads:
        copy.start()

    barrier = pltpu.get_barrier_semaphore()
    for i in range(1, devices):
        pl.semaphore_signal(
            barrier, inc=1, device_id={"tm": lax.rem(me + i, devices), "space": strip}, device_id_type=DEVICE
        )
    for i in range(1, strips):
        pl.semaphore_signal(
            barrier, inc=1, device_id={"tm": me, "space": lax.rem(strip + i, strips)}, device_id_type=DEVICE
        )
    pl.semaphore_wait(barrier, devices + strips - 2)

    down = jnp.minimum(strip + 1, strips - 1)
    up = jnp.maximum(strip - 1, 0)

    def halo_pair(index, tail, head, low_dst, high_dst):
        return (
            space_copy(tail, low_dst, zs_sem.at[index, 0], zr_sem.at[index, 0], down),
            space_copy(head, high_dst, zs_sem.at[index, 1], zr_sem.at[index, 1], up),
        )

    before_low, after_high = slice(low - TILE, low), slice(high, high + TILE)
    halos = [
        halo_pair(
            0, guess_in.at[:, rows - TILE:rows], guess_in.at[:, 0:TILE],
            guess.at[:, before_low], guess.at[:, after_high],
        ),
        halo_pair(
            1, diff_in.at[rows - TILE:rows], diff_in.at[0:TILE], diff.at[before_low], diff.at[after_high],
        ),
        halo_pair(
            2, rhs_in.at[:, rows - TILE:rows], rhs_in.at[:, 0:TILE],
            rhs.at[:, before_low], rhs.at[:, after_high],
        ),
    ]
    inside_halos = [
        halo_pair(
            3 + i, field.at[high - TILE:high], field.at[low:low + TILE], field.at[before_low], field.at[after_high],
        )
        for i, field in enumerate((g1, v1f, v1f_e))
    ]

    def start_halo(pair_of):
        @pl.when(jnp.logical_not(bottom))
        def _():
            pair_of[0].start()

        @pl.when(jnp.logical_not(top))
        def _():
            pair_of[1].start()

    def finish_halo(pair_of):
        @pl.when(jnp.logical_not(top))
        def _():
            pair_of[0].wait_recv()
            pair_of[1].wait_send()

        @pl.when(jnp.logical_not(bottom))
        def _():
            pair_of[1].wait_recv()
            pair_of[0].wait_send()

    for pair_of in halos:
        start_halo(pair_of)

    half = rows // 2
    quarter = rows // 4
    whole = [
        (low - TILE, quarter + TILE), (low + quarter, quarter),
        (low + 2 * quarter, quarter), (low + 3 * quarter, quarter + TILE),
    ]
    inner = [(low + quarter * j, quarter) for j in range(4)]
    guess_parts = [(low, half), (low + half, half), (low - TILE, TILE), (high, TILE)]

    def shift(stage, source, target, parts):
        return [
            tm_copy(
                source(start, size), target.at[start:start + size],
                ts_sem.at[stage, j], tr_sem.at[stage, j], later,
            )
            for j, (start, size) in enumerate(parts)
        ]

    def send(copy):
        @pl.when(jnp.logical_not(last))
        def _():
            copy.start()

    def receive(copy):
        @pl.when(jnp.logical_not(first))
        def _():
            copy.wait_recv()

    guess_shift = shift(
        0,
        lambda start, size: (
            guess.at[1, start:start + size] if size == TILE else guess_in.at[1, start - low:start - low + size]
        ),
        guess_e, guess_parts,
    )
    v0_shift = shift(1, lambda start, size: v0.at[1, start:start + size], v0_e, whole)
    early_shift = shift(2, lambda start, size: early.at[start:start + size], early_e, inner)
    send(guess_shift[0])
    send(guess_shift[1])

    block = [TILE]

    def at(r):
        return pl.ds(r, block[0])

    def blocks(start, size, step, init=0, ahead=0):
        def loop(begin, count, tall, carry):
            def run(i, carry):
                return step(aligned(begin + i * tall), carry)

            block[0] = tall
            if count == 1:
                carry = step(aligned(begin), carry)
            elif count:
                carry = lax.fori_loop(0, count, run, carry)
            block[0] = TILE
            return carry

        carry = loop(start, ahead // TILE, TILE, init)
        count = (size - ahead) // BLOCK
        carry = loop(start + ahead, count, BLOCK, carry)
        done = ahead + count * BLOCK
        return loop(start + done, (size - done) // TILE, TILE, carry)

    def once(start, tall, step):
        block[0] = tall
        step(aligned(start), 0)
        block[0] = TILE

    @pl.when(first)
    def _():
        def clear(r, carry):
            zero = jnp.zeros((block[0], width), jnp.float32)
            for ref in (guess_e, v0_e, v1f_e, early_e):
                ref[at(r), :] = zero
            return carry

        blocks(low - TILE, rows + 2 * TILE, clear, 0, TILE)

    def chunk(j, step, init=0):
        start, size = whole[j]
        return blocks(start, size, step, init, TILE if j == 0 else 0)

    def clear_edge(start):
        zero = jnp.zeros((TILE, width), jnp.float32)
        for ref in (guess, rhs):
            for p in range(2):
                ref[p, start:start + TILE, :] = zero
        for ref in (g1, v1f, v1f_e, diff):
            ref[start:start + TILE, :] = zero

    @pl.when(top)
    def _():
        clear_edge(low - TILE)

    @pl.when(bottom)
    def _():
        clear_edge(high)

    def stencil(tall):
        size = block[0]
        lane = lax.broadcasted_iota(jnp.int32, (size, width), 1)
        not_left, not_right = lane != 0, lane != width - 1
        mid = tall[TILE:TILE + size]
        total = tall[TILE - 1:TILE + size - 1] + tall[TILE + 1:TILE + size + 1]
        total = total + jnp.where(not_left, pltpu.roll(mid, 1, 1), 0.0)
        total = total + jnp.where(not_right, pltpu.roll(mid, width - 1, 1), 0.0)
        return mid, total

    def tall_at(r):
        return pl.ds(aligned(r - TILE), block[0] + 2 * TILE)

    def coefficients(r):
        scaled = diff[at(r), :]
        return scaled, 1.0 + 4.0 * scaled, weights[at(r), :]

    def set_weights(r, carry):
        weights[at(r), :] = damping / (1.0 + 4.0 * diff[at(r), :])
        return carry

    def squares(value, keep=None):
        square = value * value
        if keep is not None:
            square = jnp.where(keep, square, 0.0)
        total = square[:, 0:128]
        for i in range(1, width // 128):
            total = total + square[:, i * 128:(i + 1) * 128]
        folded = total[0:TILE]
        for i in range(TILE, block[0], TILE):
            folded = folded + total[i:i + TILE]
        return folded

    zero_tile = jnp.zeros((TILE, 128), jnp.float32)
    keep_share = 1.0 - damping

    def sweep_last(r, carry):
        scaled, _, weight = coefficients(r)
        mid, total = stencil(guess[1, tall_at(r), :])
        v0[1, at(r), :] = keep_share * mid + weight * (rhs[1, at(r), :] + scaled * total + guess[0, at(r), :])
        return carry

    for copy in loads:
        copy.wait()
    blocks(low, rows, set_weights)
    for j in (1, 2):
        chunk(j, sweep_last)
    finish_halo(halos[0])
    send(guess_shift[2])
    send(guess_shift[3])
    finish_halo(halos[1])
    finish_halo(halos[2])
    blocks(low - TILE, TILE, set_weights)
    blocks(high, TILE, set_weights)
    for j in (0, 3):
        chunk(j, sweep_last)
    for j in (0, 3, 1, 2):
        send(v0_shift[j])

    c_low, c_high = EDGE, EDGE + piece
    c_rows = slice(c_low - TILE, c_high + TILE)
    offset = me * piece

    def coarse(step, init=0):
        return blocks(c_low - TILE, tall_piece, step, init, TILE)

    def coarse_diff(r):
        return diff[at(aligned(r + offset)), :]

    def set_coarse_weights(r, carry):
        base = coarse_diff(r)
        for level in range(1, LEVELS):
            c_weights[level - 1, at(r), :] = damping / (1.0 + 4.0 * (2.0**level * base))
        return carry

    coarse(set_coarse_weights)

    def sweep_first(r, carry):
        scaled, _, weight = coefficients(r)
        mid, total = stencil(guess[0, tall_at(r), :])
        value = keep_share * mid + weight * (rhs[0, at(r), :] + scaled * total + guess_e[at(r), :])
        v0[0, at(r), :] = value
        early[at(r), :] = rhs[1, at(r), :] + value
        return carry

    for copy in guess_shift:
        receive(copy)
    for j in range(4):
        chunk(j, sweep_first)

    def descend(r, carry):
        scaled, diag, _ = coefficients(r)
        mid, total = stencil(v0[0, tall_at(r), :])
        one = rhs[0, at(r), :] - diag * mid + scaled * total + v0_e[at(r), :]
        late, total = stencil(v0[1, tall_at(r), :])
        two = rhs[1, at(r), :] - diag * late + scaled * total + mid
        g1[at(r), :] = one + two
        return carry + squares(one) + squares(two)

    c_g1 = c_sources[0]

    def hand_over(k):
        start = low - TILE + k * piece
        source = g1.at[start:start + tall_piece]
        return source, tm_copy(source, c_g1.at[me, c_rows], as_sem.at[k], ar_sem.at[me], k)

    def give(k):
        source, copy = hand_over(k)
        local = pltpu.make_async_copy(source, c_g1.at[me, c_rows], al_sem)

        @pl.when(me == k)
        def _():
            local.start()
            local.wait()

        @pl.when(me != k)
        def _():
            copy.start()

    total0 = zero_tile
    ready, given = [False] * 4, set()

    def covered(k):
        begin, end = max(0, k * piece - TILE), min(rows, (k + 1) * piece + TILE)
        return all(ready[j] for j in range(4) if begin < (j + 1) * quarter and end > j * quarter)

    edges = (0, devices - 1)
    for j in (0, 3, 1, 2):
        receive(v0_shift[j])
        total0 = blocks(*inner[j], descend, total0)
        ready[j] = True
        if j == 3:
            start_halo(inside_halos[0])
        for k in range(devices):
            if k not in given and k not in edges and covered(k):
                given.add(k)
                give(k)
        if j == 1:
            finish_halo(inside_halos[0])
            for k in edges:
                give(k)
    send(early_shift[0])
    send(early_shift[1])
    for s in range(devices):
        copy = tm_copy(c_g1.at[s, c_rows], c_g1.at[s, c_rows], as_sem.at[0], ar_sem.at[s], sibling)

        @pl.when(s != me)
        def _():
            copy.wait_recv()

    def coarse_coefficients(level, r):
        return 2.0**level * coarse_diff(r), c_weights[level - 1, at(r), :]

    def first_sweep(level, count):
        source, field = c_sources[level - 1], c_fields[level - 1]

        def step(r, carry):
            _, weight = coarse_coefficients(level, r)
            for p in range(count):
                field[p, at(r), :] = weight * source[p, at(r), :]
            return carry

        coarse(step)

    def coarse_residual(level, count):
        source, field, target = c_sources[level - 1], c_fields[level - 1], c_sources[level]

        def step(r, carry):
            keep = jnp.logical_and(r >= c_low, r < c_high)
            scaled, _ = coarse_coefficients(level, r)
            earlier, even = None, None
            for p in range(count):
                mid, total = stencil(field[p, tall_at(r), :])
                resid = keep_share * source[p, at(r), :] + scaled * total
                if p:
                    resid = resid + earlier
                earlier = mid
                carry = carry + squares(resid, keep)
                if p % 2 == 0:
                    even = resid
                else:
                    target[p // 2, at(r), :] = even + resid
            return carry

        return coarse(step, zero_tile)

    def ascend(level, count):
        source, field = c_sources[level - 1], c_fields[level - 1]
        above, target = c_finals[level], c_finals[level - 1]

        def step(r, carry):
            scaled, weight = coarse_coefficients(level, r)
            earlier = None
            for p in range(count):
                mid, total = stencil(field[p, tall_at(r), :] + above[p // 2, tall_at(r), :])
                value = source[p, at(r), :] + scaled * total
                if p:
                    value = value + earlier
                earlier = mid
                target[p, at(r), :] = keep_share * mid + weight * value
            return carry

        coarse(step)

    coarsest = LEVELS - 1
    parts = [total0]
    for level in range(1, coarsest):
        first_sweep(level, devices >> (level - 1))
        parts.append(coarse_residual(level, devices >> (level - 1)))
    first_sweep(coarsest, 1)

    source_l, field_l, final_l = c_sources[coarsest - 1], c_fields[coarsest - 1], c_finals[coarsest - 1]

    def second_sweep(r, carry):
        scaled, weight = coarse_coefficients(coarsest, r)
        mid, total = stencil(field_l[0, tall_at(r), :])
        final_l[0, at(r), :] = keep_share * mid + weight * (source_l[0, at(r), :] + scaled * total)
        return carry

    coarse(second_sweep)
    for level in range(coarsest - 1, 1, -1):
        ascend(level, devices >> (level - 1))

    c_v1, c_v2f, c_v1f = c_fields[0], c_finals[1], c_finals[0]
    back = []
    place = pl.ds(aligned(low + offset), piece)

    def give_back(kind, target, point, dst):
        src = c_v1f.at[point, c_low:c_high]
        copy = tm_copy(src, dst.at[place], bs_sem.at[kind, target], br_sem.at[kind, me], target)
        local = pltpu.make_async_copy(src, dst.at[place], bl_sem.at[kind])
        back.append((target, copy))

        @pl.when(me == target)
        def _():
            local.start()
            local.wait()

        @pl.when(me != target)
        def _():
            copy.start()

    block[0] = piece
    scaled, weight = coarse_coefficients(1, c_low)
    for p in range(devices):
        mid, total = stencil(c_v1[p, tall_at(c_low), :] + c_v2f[p // 2, tall_at(c_low), :])
        value = c_g1[p, at(c_low), :] + scaled * total
        if p:
            value = value + (c_v1[p - 1, at(c_low), :] + c_v2f[(p - 1) // 2, at(c_low), :])
        c_v1f[p, at(c_low), :] = keep_share * mid + weight * value
        give_back(0, p, p, v1f)
    block[0] = TILE
    for p in range(2, devices, 2):
        give_back(1, p, p - 1, v1f_e)
    send(early_shift[2])
    send(early_shift[3])

    def residual_l(r, carry):
        scaled = 2.0**coarsest * coarse_diff(r)
        mid, total = stencil(final_l[0, tall_at(r), :])
        return carry + squares(source_l[0, at(r), :] - (1.0 + 4.0 * scaled) * mid + scaled * total)

    parts.append(blocks(c_low, piece, residual_l, zero_tile))

    order = [0, devices - 1] + list(range(1, devices - 1))

    def rows_of(k):
        return slice(low + k * piece, low + (k + 1) * piece)

    def relay(k):
        return tm_copy(v1f.at[rows_of(k)], v1f_e.at[rows_of(k)], rs_sem.at[k], br_sem.at[1, k], sibling)

    for i, k in enumerate(order):
        arrival = tm_copy(v1f.at[rows_of(k)], v1f.at[rows_of(k)], rs_sem.at[k], br_sem.at[0, k], sibling)

        @pl.when(k != me)
        def _():
            arrival.wait_recv()

        @pl.when(core == 0)
        def _():
            relay(k).start()

        if i == 1:
            start_halo(inside_halos[1])

    def ascend_last(r, carry):
        scaled, _, weight = coefficients(r)
        mid, total = stencil(v0[1, tall_at(r), :] + v1f[tall_at(r), :])
        earlier = v0[0, at(r), :] + v1f[at(r), :]
        sol[1, at(r), :] = keep_share * mid + weight * (rhs[1, at(r), :] + scaled * total + earlier)
        return carry

    blocks(low + TILE, rows - 2 * TILE, ascend_last)
    finish_halo(inside_halos[1])
    once(low - TILE, 2 * TILE, ascend_last)
    once(high - TILE, 2 * TILE, ascend_last)

    for i, k in enumerate(order):
        @pl.when(jnp.logical_and(jnp.logical_not(first), jnp.logical_or(core == 1, k != me)))
        def _():
            relay(k).wait_recv()

        if i == 1:
            @pl.when(jnp.logical_not(first))
            def _():
                start_halo(inside_halos[2])

    def ascend_first(r, carry):
        scaled, _, weight = coefficients(r)
        mid, total = stencil(v0[0, tall_at(r), :] + v1f[tall_at(r), :])
        earlier = v0_e[at(r), :] + v1f_e[at(r), :]
        sol[0, at(r), :] = keep_share * mid + weight * (rhs[0, at(r), :] + scaled * total + earlier)
        return carry

    blocks(low + TILE, rows - 2 * TILE, ascend_first)

    @pl.when(jnp.logical_not(first))
    def _():
        finish_halo(inside_halos[2])

    once(low - TILE, 2 * TILE, ascend_first)
    once(high - TILE, 2 * TILE, ascend_first)
    stores = pltpu.make_async_copy(sol.at[:, low:high], out, store_sem)
    stores.start()

    def final_last(r, carry):
        scaled, diag, _ = coefficients(r)
        mid, total = stencil(sol[1, tall_at(r), :])
        return carry + squares(rhs[1, at(r), :] - diag * mid + scaled * total + sol[0, at(r), :])

    total5 = blocks(low, rows, final_last, zero_tile)

    def final_first(r, carry):
        scaled, diag, weight = coefficients(r)
        before = v1f_e[at(r), :]
        mid, total = stencil(v0_e[tall_at(r), :] + v1f_e[tall_at(r), :])
        sol_e = keep_share * mid + weight * (early_e[at(r), :] + scaled * total + before)
        mid, total = stencil(sol[0, tall_at(r), :])
        return carry + squares(rhs[0, at(r), :] - diag * mid + scaled * total + sol_e)

    for (start, size), arrived in zip(inner, early_shift):
        receive(arrived)
        total5 = blocks(start, size, final_first, total5)

    parts.append(total5)
    for level, value in enumerate(parts):
        tile[level:level + 1, :] = jnp.sum(value, axis=0, keepdims=True)
    for level in range(len(parts), TILE):
        tile[level:level + 1, :] = jnp.zeros((1, 128), jnp.float32)

    def exchange(count, own, source, slots, copier, send_sems, recv_sems):
        slots[pl.ds(own, 1)] = source[...][None]
        sent = [
            copier(source, slots.at[own], send_sems.at[i], recv_sems.at[own], lax.rem(own + i, count))
            for i in range(1, count)
        ]
        for copy in sent:
            copy.start()
        for i in range(1, count):
            other = lax.rem(own + i, count)
            copier(source, slots.at[other], send_sems.at[i], recv_sems.at[other], other).wait_recv()
        for copy in sent:
            copy.wait_send()
        total = slots[0]
        for i in range(1, count):
            total = total + slots[i]
        return total

    total = exchange(devices, me, tile, gathered, tm_copy, ns_sem, nr_sem)
    tile[...] = total
    total = exchange(strips, strip, tile, gathered_z, space_copy, ms_sem, mr_sem)
    summed = jnp.sum(total, axis=1, keepdims=True)
    norms_out[...] = jnp.broadcast_to(jnp.sqrt(summed * (1.0 / cells)), (TILE, 128))

    stores.wait()
    for group in (guess_shift, v0_shift, early_shift):
        for copy in group:
            @pl.when(jnp.logical_not(last))
            def _():
                copy.wait_send()
    for k in range(devices):
        @pl.when(me != k)
        def _():
            hand_over(k)[1].wait_send()

        @pl.when(core == 0)
        def _():
            relay(k).wait_send()
    for target, copy in back:
        @pl.when(me != target)
        def _():
            copy.wait_send()


def fast_body(rhs, guess, diffusion):
    devices, strips = lax.axis_size("tm"), lax.axis_size("space")
    rows, width = rhs.shape[1:]
    cells = rows * strips * width
    height = rows + 2 * EDGE
    c_height = rows // devices + 2 * EDGE

    def plane(*lead):
        return pltpu.VMEM(lead + (height, width), jnp.float32)

    def coarse(count):
        return pltpu.VMEM((count, c_height, width), jnp.float32)

    def pyramid():
        return tuple(coarse(devices >> level) for level in range(LEVELS - 1))

    dma = pltpu.SemaphoreType.DMA
    scratch = [
        plane(2), plane(2), plane(), plane(2), plane(), plane(), plane(2),
        plane(), plane(), plane(), plane(), plane(), plane(),
        coarse(LEVELS - 1), pyramid(), pyramid(), pyramid(),
        pltpu.VMEM((TILE, 128), jnp.float32),
        pltpu.VMEM((devices, TILE, 128), jnp.float32),
        pltpu.VMEM((strips, TILE, 128), jnp.float32),
        dma((3,)), dma, dma((6, 2)), dma((6, 2)), dma((3, 4)), dma((3, 4)), dma((devices,)), dma((devices,)), dma,
        dma((2, devices)), dma((2, devices)), dma((2,)), dma((devices,)),
        dma((devices,)), dma((devices,)), dma((strips,)), dma((strips,)),
    ]
    any_space = pl.BlockSpec(memory_space=pl.ANY)
    result, norms = pl.pallas_call(
        functools.partial(cycle_kernel, strips, devices, cells),
        out_shape=(
            pltpu.VMEM(rhs.shape, jnp.float32),
            jax.ShapeDtypeStruct((TILE, 128), jnp.float32),
        ),
        in_specs=[any_space] * 3,
        out_specs=(pl.BlockSpec(memory_space=pltpu.VMEM), pl.BlockSpec(memory_space=pltpu.VMEM)),
        scratch_shapes=scratch,
        compiler_params=pltpu.CompilerParams(
            collective_id=0, has_side_effects=True, vmem_limit_bytes=67_043_328 - rhs.size * 4 - 2**17
        ),
    )(rhs, guess, diffusion)
    return result, norms[:LEVELS + 1, 0]


def solution(mesh):
    in_specs = (P("tm", "space", None), P("tm", "space", None), P("space", None))
    out_specs = (P("tm", "space", None), P())

    def choose(rhs, guess, diffusion):
        points = rhs.shape[0] * lax.axis_size("tm")
        one_coarsest = points == 2 ** (LEVELS - 1) and rhs.shape[0] == 2
        even = rhs.shape[1] % (TILE * lax.axis_size("tm")) == 0 and rhs.shape[2] % 128 == 0
        if one_coarsest and even:
            return fast_body(rhs, guess, diffusion)
        return body(rhs, guess, diffusion)

    return jax.shard_map(choose, mesh=mesh, in_specs=in_specs, out_specs=out_specs, check_vma=False)
```

```python
import functools

import jax
import jax.numpy as jnp
from jax import lax
from jax.experimental import pallas as pl
from jax.experimental.pallas import tpu as pltpu
from jax.sharding import PartitionSpec as P

LEVELS = 5


damping = 0.8


def with_halo(block, sides, width):
    for axis, dim in sides:
        count = lax.axis_size(axis)
        forward = [(i, i + 1) for i in range(count - 1)]
        backward = [(target, source) for source, target in forward]
        low = lax.ppermute(
            lax.slice_in_dim(block, block.shape[dim] - width, None, axis=dim), axis, forward
        )
        high = lax.ppermute(lax.slice_in_dim(block, 0, width, axis=dim), axis, backward)
        block = jnp.concatenate([low, block, high], axis=dim)
    return block


def shifted(value, axis, steps):
    count = lax.axis_size(axis)
    first, last = (max(0, -steps), min(count, count - steps))
    return lax.ppermute(value, axis, [(source, source + steps) for source in range(first, last)])


def from_partner(value, axis, apart):
    mask = 2**apart
    pairs = [(source, source ^ mask) for source in range(lax.axis_size(axis))]
    return lax.ppermute(value, axis, pairs)


def neighbours(field):
    rows = with_halo(field, (("space", 1),), 1)
    padded = jnp.pad(rows, ((0, 0), (0, 0), (1, 1)))
    total = padded[:, 2:, 1:-1] + padded[:, :-2, 1:-1]
    total = total + padded[:, 1:-1, 2:] + padded[:, 1:-1, :-2]
    return total


def residual(field, source, scaled, diag, stride):
    earlier = shifted(field[-1:], "tm", stride)
    before = jnp.concatenate([earlier, field[:-1]], axis=0)
    image = diag * field - scaled * neighbours(field) - before
    return source - image


def stride_of(level):
    if level == 0:
        return 1
    return 2 ** (level - 1)


def body(rhs, guess, diffusion):
    position = lax.axis_index("tm")
    cells = rhs.shape[1] * lax.axis_size("space") * rhs.shape[2]
    partials = []

    def weight_of(level):
        if level <= 1:
            return jnp.float32(1.0)
        stride = stride_of(level)
        return jnp.where(position % stride == stride - 1, 1.0, 0.0).astype(jnp.float32)

    def record(resid, level):
        local_part = jnp.sum(resid * resid) * weight_of(level)
        partials.append(local_part)

    sources = [rhs]
    fields = []
    field = guess
    for level in range(LEVELS - 1):
        source = sources[level]
        scaled = 2.0**level * diffusion
        diag = 1.0 + 4.0 * scaled
        stride = stride_of(level)
        if level == 0:
            field = field + damping * residual(field, source, scaled, diag, stride) / diag
        else:
            field = damping * source / diag
        resid = residual(field, source, scaled, diag, stride)
        record(resid, level)
        fields.append(field)
        if level == 0:
            coarse = resid[0:1] + resid[1:2]
        else:
            coarse = resid + from_partner(resid, "tm", level - 1)
        sources.append(coarse)
    level = LEVELS - 1
    source = sources[level]
    scaled = 2.0**level * diffusion
    diag = 1.0 + 4.0 * scaled
    stride = stride_of(level)
    field = damping * source / diag
    field = field + damping * residual(field, source, scaled, diag, stride) / diag
    resid = residual(field, source, scaled, diag, stride)
    record(resid, level)
    correction = field
    for level in range(LEVELS - 2, -1, -1):
        scaled = 2.0**level * diffusion
        diag = 1.0 + 4.0 * scaled
        stride = stride_of(level)
        field = fields[level] + correction
        field = field + damping * residual(field, sources[level], scaled, diag, stride) / diag
        correction = field
    scaled = 1.0 * diffusion
    diag = 1.0 + 4.0 * scaled
    resid = residual(correction, rhs, scaled, diag, 1)
    record(resid, 0)
    totals = lax.psum(jnp.stack(partials), ("tm", "space"))
    norms = jnp.sqrt(totals / cells)
    return (correction, norms)


DEVICE = pl.DeviceIdType.MESH
TILE = 8
EDGE = 2 * TILE
BLOCK = 64
EARLY = 2
LANES = 128


def cycle_kernel(
    strips, devices, cells,
    rhs_in, guess_in, diff_in, out, norms_out,
    rhs, guess, diff, v0, v1, v1f, sol, guess_e, v0_e, v1f_e, early, early_e, weights,
    c_weights, c_fields, c_sums, c_top, c_v1f, tile, gathered, gathered_z,
    load_sem, zs_sem, zr_sem, ts_sem, tr_sem, as_sem, ar_sem, al_sem,
    bs_sem, br_sem, bl_sem, rs_sem, ns_sem, nr_sem, ms_sem, mr_sem,
):
    me = lax.axis_index("tm")
    strip = lax.axis_index("space")
    rows, width = rhs_in.shape[1], rhs_in.shape[2]
    tiles = width // LANES
    core = lax.rem(me, 2)
    sibling = me + 1 - 2 * core
    low, high = EDGE, EDGE + rows
    first, last = me == 0, me == devices - 1
    top, bottom = strip == 0, strip == strips - 1
    piece = rows // devices
    tall_piece = piece + 2 * TILE

    def aligned(value):
        return pl.multiple_of(value, TILE)

    def tm_copy(src, dst, send, recv, target):
        return pltpu.make_async_remote_copy(
            src_ref=src, dst_ref=dst, send_sem=send, recv_sem=recv,
            device_id={"tm": target, "space": strip}, device_id_type=DEVICE,
        )

    def space_copy(src, dst, send, recv, target):
        return pltpu.make_async_remote_copy(
            src_ref=src, dst_ref=dst, send_sem=send, recv_sem=recv,
            device_id={"tm": me, "space": target}, device_id_type=DEVICE,
        )

    later = jnp.minimum(me + 1, devices - 1)
    inside = slice(low, high)

    def load(index, source, target):
        return [
            pltpu.make_async_copy(
                source.at[:, j * LANES:(j + 1) * LANES], target.at[j, inside], load_sem.at[index, j]
            )
            for j in range(tiles)
        ]

    loads = [
        load(0, guess_in.at[1], guess.at[1]), load(1, guess_in.at[0], guess.at[0]), load(2, diff_in, diff),
        load(3, rhs_in.at[1], rhs.at[1]), load(4, rhs_in.at[0], rhs.at[0]),
    ]
    for group in loads:
        for copy in group:
            copy.start()

    barrier = pltpu.get_barrier_semaphore()
    for i in range(1, devices):
        pl.semaphore_signal(
            barrier, inc=1, device_id={"tm": lax.rem(me + i, devices), "space": strip}, device_id_type=DEVICE
        )
    for i in range(1, strips):
        pl.semaphore_signal(
            barrier, inc=1, device_id={"tm": me, "space": lax.rem(strip + i, strips)}, device_id_type=DEVICE
        )

    def row_tiles(start, size):
        return [start + i * TILE for i in range(size // TILE)]

    def blocks(start, size, step, carry=0):
        count = size // BLOCK

        def run(i, carry):
            begin = aligned(start + i * BLOCK)
            for offset in range(0, BLOCK, TILE):
                carry = step(begin + offset, carry)
            return carry

        if count == 1:
            carry = run(0, carry)
        elif count:
            carry = lax.fori_loop(0, count, run, carry)
        for r in row_tiles(start + count * BLOCK, size - count * BLOCK):
            carry = step(r, carry)
        return carry

    def at(r):
        return pl.ds(r, TILE)

    zero = jnp.zeros((TILE, LANES), jnp.float32)

    @pl.when(first)
    def _():
        def clear(r, carry):
            for ref in (guess_e, v0_e, v1f_e, early_e):
                for j in range(tiles):
                    ref[j, at(r), :] = zero
            return carry

        blocks(low - TILE, rows + 2 * TILE, clear)

    def clear_edge(start):
        for j in range(tiles):
            for ref in (guess, rhs):
                for p in range(2):
                    ref[p, j, start:start + TILE, :] = zero
            for ref in (v1, v1f, v1f_e, diff):
                ref[j, start:start + TILE, :] = zero

    @pl.when(top)
    def _():
        clear_edge(low - TILE)

    @pl.when(bottom)
    def _():
        clear_edge(high)

    pl.semaphore_wait(barrier, devices + strips - 2)

    down = jnp.minimum(strip + 1, strips - 1)
    up = jnp.maximum(strip - 1, 0)

    def halo_pair(index, field, lead=()):
        def rows_at(start):
            return field.at[lead + (slice(None), slice(start, start + TILE))]

        return (
            space_copy(rows_at(high - TILE), rows_at(low - TILE), zs_sem.at[index, 0], zr_sem.at[index, 0], down),
            space_copy(rows_at(low), rows_at(high), zs_sem.at[index, 1], zr_sem.at[index, 1], up),
        )

    guess_halo = halo_pair(0, guess, (slice(None),))
    diff_halo = halo_pair(1, diff)
    rhs_halo = halo_pair(2, rhs, (slice(None),))
    v1_halo, v1f_halo, v1f_e_halo = [halo_pair(3 + i, field) for i, field in enumerate((v1, v1f, v1f_e))]

    def start_halo(pair_of):
        @pl.when(jnp.logical_not(bottom))
        def _():
            pair_of[0].start()

        @pl.when(jnp.logical_not(top))
        def _():
            pair_of[1].start()

    def finish_halo(pair_of):
        @pl.when(jnp.logical_not(top))
        def _():
            pair_of[0].wait_recv()
            pair_of[1].wait_send()

        @pl.when(jnp.logical_not(bottom))
        def _():
            pair_of[1].wait_recv()
            pair_of[0].wait_send()

    half = rows // 2
    quarter = rows // 4
    whole = [
        (low - TILE, quarter + TILE), (low + quarter, quarter),
        (low + 2 * quarter, quarter), (low + 3 * quarter, quarter + TILE),
    ]
    inner = [(low + quarter * j, quarter) for j in range(4)]
    guess_parts = [(low, half), (low + half, half), (low - TILE, TILE), (high, TILE)]

    def shift(stage, source, target, parts):
        return [
            tm_copy(
                source.at[:, start:start + size], target.at[:, start:start + size],
                ts_sem.at[stage, j], tr_sem.at[stage, j], later,
            )
            for j, (start, size) in enumerate(parts)
        ]

    def send(copy):
        @pl.when(jnp.logical_not(last))
        def _():
            copy.start()

    def receive(copy):
        @pl.when(jnp.logical_not(first))
        def _():
            copy.wait_recv()

    guess_shift = shift(0, guess.at[1], guess_e, guess_parts)
    v0_shift = shift(1, v0.at[1], v0_e, whole)
    early_shift = shift(2, early, early_e, inner)

    for copy in loads[0]:
        copy.wait()
    send(guess_shift[0])
    send(guess_shift[1])
    for copy in loads[1]:
        copy.wait()
    start_halo(guess_halo)
    for copy in loads[2]:
        copy.wait()
    start_halo(diff_halo)
    for copy in loads[3] + loads[4]:
        copy.wait()
    start_halo(rhs_halo)

    lane = lax.broadcasted_iota(jnp.int32, (TILE, LANES), 1)
    at_left, at_right = lane == 0, lane == LANES - 1

    def stencil(field, r):
        mids = [field[j, at(r), :] for j in range(tiles)]
        right = [zero] + [pltpu.roll(mid, 1, 1) for mid in mids]
        left = [pltpu.roll(mid, LANES - 1, 1) for mid in mids] + [zero]
        totals = []
        for j in range(tiles):
            total = field[j, at(r - 1), :] + field[j, at(r + 1), :]
            total = total + jnp.where(at_left, right[j], right[j + 1])
            totals.append(total + jnp.where(at_right, left[j + 1], left[j]))
        return mids, totals

    def squares(values):
        total = values[0] * values[0]
        for value in values[1:]:
            total = total + value * value
        return total

    keep_share = 1.0 - damping

    def set_weights(r, carry):
        for j in range(tiles):
            scaled = diff[j, at(r), :]
            for level in range(2):
                weights[level, j, at(r), :] = damping / (1.0 + 4.0 * (2.0**level * scaled))
        return carry

    def sweep(p, source, before, target, also=None):
        def step(r, carry):
            mids, totals = stencil(source, r)
            for j in range(tiles):
                inner_sum = rhs[p, j, at(r), :] + diff[j, at(r), :] * totals[j] + before[j, at(r), :]
                value = keep_share * mids[j] + weights[0, j, at(r), :] * inner_sum
                target[j, at(r), :] = value
                if also is not None:
                    also(j, r, value)
            return carry

        return step

    def level_residual(p, j, r, mid, total, before):
        scaled = diff[j, at(r), :]
        return rhs[p, j, at(r), :] - mid + scaled * (total - 4.0 * mid) + before

    sweep_last = sweep(1, guess.at[1], guess.at[0], v0.at[1])
    blocks(low, rows, set_weights)
    blocks(low + quarter, 2 * quarter, sweep_last)
    finish_halo(guess_halo)
    send(guess_shift[2])
    send(guess_shift[3])
    finish_halo(diff_halo)
    finish_halo(rhs_halo)
    set_weights(low - TILE, 0)
    set_weights(high, 0)
    for j in (0, 3):
        blocks(*whole[j], sweep_last)
    for j in (0, 3, 1, 2):
        send(v0_shift[j])

    c_low, c_high = EDGE, EDGE + piece
    c_rows = slice(c_low - TILE, c_high + TILE)
    c_tiles, c_own = row_tiles(c_low - TILE, tall_piece), row_tiles(c_low, piece)
    offset = me * piece

    def coarse_diff(j, r):
        return diff[j, at(aligned(r + offset)), :]

    def coarse_weights(i, carry):
        r = aligned(c_low - TILE + i * TILE)
        for j in range(tiles):
            base = coarse_diff(j, r)
            for level in range(1, LEVELS):
                c_weights[level - 1, j, at(r), :] = damping / (1.0 + 4.0 * (2.0**level * base))
        return carry

    lax.fori_loop(0, tall_piece // TILE, coarse_weights, 0)

    def keep_early(j, r, value):
        early[j, at(r), :] = rhs[1, j, at(r), :] + value

    for copy in guess_shift:
        receive(copy)
    blocks(low - TILE, rows + 2 * TILE, sweep(0, guess.at[0], guess_e, v0.at[0], keep_early))

    def descend(r, carry):
        firsts, totals = stencil(v0.at[0], r)
        lasts, totals_last = stencil(v0.at[1], r)
        ones, twos = [], []
        for j in range(tiles):
            ones.append(level_residual(0, j, r, firsts[j], totals[j], v0_e[j, at(r), :]))
            twos.append(level_residual(1, j, r, lasts[j], totals_last[j], firsts[j]))
            v1[j, at(r), :] = weights[1, j, at(r), :] * (ones[j] + twos[j])
        return carry + (squares(ones) + squares(twos))

    c_v1 = c_fields[0]

    def hand_over(k):
        start = low - TILE + k * piece
        source = v1.at[:, start:start + tall_piece]
        return source, tm_copy(source, c_v1.at[me, :, c_rows], as_sem.at[k], ar_sem.at[me], k)

    def give(k):
        source, copy = hand_over(k)
        local = pltpu.make_async_copy(source, c_v1.at[me, :, c_rows], al_sem)

        @pl.when(me == k)
        def _():
            local.start()
            local.wait()

        @pl.when(me != k)
        def _():
            copy.start()

    total0 = zero
    ready, given = [False] * 4, set()

    def covered(k):
        begin, end = max(0, k * piece - TILE), min(rows, (k + 1) * piece + TILE)
        return all(ready[j] for j in range(4) if begin < (j + 1) * quarter and end > j * quarter)

    edges = (0, devices - 1)
    for j in (0, 3, 1, 2):
        receive(v0_shift[j])
        total0 = blocks(*inner[j], descend, total0)
        ready[j] = True
        if j == 3:
            start_halo(v1_halo)
        for k in range(devices):
            if k not in given and k not in edges and covered(k):
                given.add(k)
                give(k)
        if j == 1:
            finish_halo(v1_halo)
            for k in edges:
                give(k)
    for copy in early_shift[:EARLY]:
        send(copy)
    for s in range(devices):
        copy = tm_copy(c_v1.at[s, :, c_rows], c_v1.at[s, :, c_rows], as_sem.at[0], ar_sem.at[s], sibling)

        @pl.when(s != me)
        def _():
            copy.wait_recv()

    coarsest = LEVELS - 1

    def coarse_residual(level):
        field, target = c_fields[level - 1], c_fields[level]
        count = devices >> (level - 1)
        carry = zero
        for r in c_tiles:
            own = c_low <= r < c_high
            scaled = [2.0**level * coarse_diff(j, r) for j in range(tiles)]
            earlier, even = None, None
            for p in range(count):
                mids, totals = stencil(field.at[p], r)
                resid = []
                for j in range(tiles):
                    value = 0.25 * mids[j] + scaled[j] * (mids[j] + totals[j])
                    resid.append(value + earlier[j] if p else value)
                earlier = mids
                if own:
                    carry = carry + squares(resid)
                if p % 2 == 0:
                    even = resid
                else:
                    for j in range(tiles):
                        target[p // 2, j, at(r), :] = c_weights[level, j, at(r), :] * (even[j] + resid[j])
        return carry

    def lift(level, p, j, r, value):
        for q in (2 * p, 2 * p + 1):
            c_sums[level - 1][q, j, at(r), :] = c_fields[level - 1][q, j, at(r), :] + value

    def coarse_final(level, p, r, mids, totals, scaled, earlier):
        values = []
        for j in range(tiles):
            value = scaled[j] * totals[j]
            if p:
                value = value + earlier[j]
            value = c_fields[level - 1][p, j, at(r), :] + c_weights[level - 1, j, at(r), :] * value
            values.append(keep_share * mids[j] + value)
        return values

    parts = [total0]
    for level in range(1, coarsest):
        parts.append(coarse_residual(level))

    field_l = c_fields[coarsest - 1].at[0]
    for r in c_tiles:
        mids, totals = stencil(field_l, r)
        for j in range(tiles):
            scaled = 2.0**coarsest * coarse_diff(j, r)
            value = (1.0 + keep_share) * mids[j] + c_weights[coarsest - 1, j, at(r), :] * (scaled * totals[j])
            c_top[j, at(r), :] = value
            lift(coarsest - 1, 0, j, r, value)
    for level in range(coarsest - 1, 1, -1):
        for r in c_tiles:
            scaled = [2.0**level * coarse_diff(j, r) for j in range(tiles)]
            earlier = None
            for p in range(devices >> (level - 1)):
                mids, totals = stencil(c_sums[level - 1].at[p], r)
                values = coarse_final(level, p, r, mids, totals, scaled, earlier)
                earlier = mids
                for j in range(tiles):
                    lift(level - 1, p, j, r, values[j])

    back = []
    place = pl.ds(aligned(low + offset), piece)

    def give_back(kind, target, point, field):
        src, dst = c_v1f.at[point, :, c_low:c_high], field.at[:, place]
        copy = tm_copy(src, dst, bs_sem.at[kind, target], br_sem.at[kind, me], target)
        local = pltpu.make_async_copy(src, dst, bl_sem.at[kind])
        back.append((target, copy))

        @pl.when(me == target)
        def _():
            local.start()
            local.wait()

        @pl.when(me != target)
        def _():
            copy.start()

    for part in range(0, devices, devices // 2):
        for r in c_own:
            scaled = [2.0 * coarse_diff(j, r) for j in range(tiles)]
            earlier = None
            if part:
                earlier = [c_sums[0][part - 1, j, at(r), :] for j in range(tiles)]
            for p in range(part, part + devices // 2):
                mids, totals = stencil(c_sums[0].at[p], r)
                values = coarse_final(1, p, r, mids, totals, scaled, earlier)
                earlier = mids
                for j in range(tiles):
                    c_v1f[p, j, at(r), :] = values[j]
        for p in range(part, part + devices // 2):
            give_back(0, p, p, v1f)
    for p in range(2, devices, 2):
        give_back(1, p, p - 1, v1f_e)
    for copy in early_shift[EARLY:]:
        send(copy)

    total_l = zero
    for r in c_own:
        mids, totals = stencil(c_top, r)
        resid = []
        for j in range(tiles):
            scaled = 2.0**coarsest * coarse_diff(j, r)
            ahead = (1.0 + keep_share / damping) * field_l[j, at(r), :] - mids[j]
            resid.append((1.0 + 4.0 * scaled) * ahead + scaled * totals[j])
        total_l = total_l + squares(resid)
    parts.append(total_l)

    @pl.when(jnp.logical_not(last))
    def _():
        for copy in v0_shift:
            copy.wait_send()

    order = [0, devices - 1] + list(range(1, devices - 1))

    def rows_of(k):
        return slice(low + k * piece, low + (k + 1) * piece)

    def relay(k):
        return tm_copy(v1f.at[:, rows_of(k)], v1f_e.at[:, rows_of(k)], rs_sem.at[k], br_sem.at[1, k], sibling)

    def absorb(fields, change, spots):
        for r in spots:
            for j in range(tiles):
                value = change[j, at(r), :]
                for field in fields:
                    field[j, at(r), :] = field[j, at(r), :] + value

    halo_tiles = (low - TILE, high)

    for i, k in enumerate(order):
        spots = v1f.at[:, rows_of(k)]
        arrival = tm_copy(spots, spots, rs_sem.at[k], br_sem.at[0, k], sibling)

        @pl.when(k != me)
        def _():
            arrival.wait_recv()

        @pl.when(core == 0)
        def _():
            relay(k).start()

        if i == 1:
            start_halo(v1f_halo)
        absorb((v0.at[0], v0.at[1]), v1f, row_tiles(low + k * piece, piece))

    def result(p):
        def store(j, r, value):
            out[p, at(r - low), j * LANES:(j + 1) * LANES] = value

        return store

    def ascend(p, before, finish):
        def final_sweep(store=None):
            return sweep(p, v0.at[p], before, sol.at[p], store)

        store = result(p)
        blocks(low + TILE, rows - 2 * TILE, final_sweep(store))
        finish()
        for r in halo_tiles:
            final_sweep()(r, 0)
        for r in (low, high - TILE):
            final_sweep(store)(r, 0)

    def finish_last():
        finish_halo(v1f_halo)
        absorb((v0.at[0], v0.at[1]), v1f, halo_tiles)

    ascend(1, v0.at[0], finish_last)

    for i, k in enumerate(order):
        @pl.when(jnp.logical_and(jnp.logical_not(first), jnp.logical_or(core == 1, k != me)))
        def _():
            relay(k).wait_recv()

        if i == 1:
            @pl.when(jnp.logical_not(first))
            def _():
                start_halo(v1f_e_halo)
        absorb((v0_e,), v1f_e, row_tiles(low + k * piece, piece))

    def finish_first():
        @pl.when(jnp.logical_not(first))
        def _():
            finish_halo(v1f_e_halo)

        absorb((v0_e,), v1f_e, halo_tiles)

    ascend(0, v0_e, finish_first)

    def final_last(r, carry):
        mids, totals = stencil(sol.at[1], r)
        return carry + squares([
            level_residual(1, j, r, mids[j], totals[j], sol[0, j, at(r), :]) for j in range(tiles)
        ])

    total5 = blocks(low, rows, final_last, zero)

    def final_first(r, carry):
        mids, totals = stencil(v0_e, r)
        befores = []
        for j in range(tiles):
            inner_sum = early_e[j, at(r), :] + v1f_e[j, at(r), :] + diff[j, at(r), :] * totals[j]
            befores.append(keep_share * mids[j] + weights[0, j, at(r), :] * inner_sum)
        mids, totals = stencil(sol.at[0], r)
        return carry + squares([
            level_residual(0, j, r, mids[j], totals[j], befores[j]) for j in range(tiles)
        ])

    for copy in early_shift:
        receive(copy)
    total5 = blocks(low, rows, final_first, total5)

    parts.append(total5)
    for level, value in enumerate(parts):
        tile[level:level + 1, :] = jnp.sum(value, axis=0, keepdims=True)
    for level in range(len(parts), TILE):
        tile[level:level + 1, :] = jnp.zeros((1, LANES), jnp.float32)

    def exchange(count, own, source, slots, copier, send_sems, recv_sems):
        slots[pl.ds(own, 1)] = source[...][None]
        sent = [
            copier(source, slots.at[own], send_sems.at[i], recv_sems.at[own], lax.rem(own + i, count))
            for i in range(1, count)
        ]
        for copy in sent:
            copy.start()
        for i in range(1, count):
            other = lax.rem(own + i, count)
            copier(source, slots.at[other], send_sems.at[i], recv_sems.at[other], other).wait_recv()
        for copy in sent:
            copy.wait_send()
        total = slots[0]
        for i in range(1, count):
            total = total + slots[i]
        return total

    total = exchange(devices, me, tile, gathered, tm_copy, ns_sem, nr_sem)
    tile[...] = total
    total = exchange(strips, strip, tile, gathered_z, space_copy, ms_sem, mr_sem)
    summed = jnp.sum(total, axis=1, keepdims=True)
    norms_out[...] = jnp.broadcast_to(jnp.sqrt(summed * (1.0 / cells)), (TILE, LANES))

    @pl.when(jnp.logical_not(last))
    def _():
        for copy in guess_shift + early_shift:
            copy.wait_send()

    for k in range(devices):
        @pl.when(me != k)
        def _():
            hand_over(k)[1].wait_send()

        @pl.when(core == 0)
        def _():
            relay(k).wait_send()
    for target, copy in back:
        @pl.when(me != target)
        def _():
            copy.wait_send()


def fast_body(rhs, guess, diffusion):
    devices, strips = lax.axis_size("tm"), lax.axis_size("space")
    rows, width = rhs.shape[1:]
    tiles = width // LANES
    cells = rows * strips * width

    def spread(height):
        return height + (TILE - height) % (4 * TILE)

    def plane(*lead):
        return pltpu.VMEM(lead + (tiles, spread(rows + 2 * EDGE), LANES), jnp.float32)

    def coarse(*lead):
        return pltpu.VMEM(lead + (tiles, spread(rows // devices + 2 * EDGE), LANES), jnp.float32)

    dma = pltpu.SemaphoreType.DMA
    scratch = [
        plane(2), plane(2), plane(), plane(2), plane(), plane(), plane(2),
        plane(), plane(), plane(), plane(), plane(), plane(2),
        coarse(LEVELS - 1), tuple(coarse(devices >> level) for level in range(LEVELS - 1)),
        tuple(coarse(devices >> level) for level in range(LEVELS - 2)), coarse(), coarse(devices),
        pltpu.VMEM((TILE, LANES), jnp.float32),
        pltpu.VMEM((devices, TILE, LANES), jnp.float32),
        pltpu.VMEM((strips, TILE, LANES), jnp.float32),
        dma((5, tiles)), dma((6, 2)), dma((6, 2)), dma((3, 4)), dma((3, 4)), dma((devices,)), dma((devices,)), dma,
        dma((2, devices)), dma((2, devices)), dma((2,)), dma((devices,)),
        dma((devices,)), dma((devices,)), dma((strips,)), dma((strips,)),
    ]
    any_space = pl.BlockSpec(memory_space=pl.ANY)
    result, norms = pl.pallas_call(
        functools.partial(cycle_kernel, strips, devices, cells),
        out_shape=(
            pltpu.VMEM(rhs.shape, jnp.float32),
            jax.ShapeDtypeStruct((TILE, LANES), jnp.float32),
        ),
        in_specs=[any_space] * 3,
        out_specs=(pl.BlockSpec(memory_space=pltpu.VMEM), pl.BlockSpec(memory_space=pltpu.VMEM)),
        scratch_shapes=scratch,
        compiler_params=pltpu.CompilerParams(
            collective_id=0, has_side_effects=True, vmem_limit_bytes=67_043_328 - rhs.size * 4 - 2**17
        ),
    )(rhs, guess, diffusion)
    return result, norms[:LEVELS + 1, 0]


def solution(mesh):
    in_specs = (P("tm", "space", None), P("tm", "space", None), P("space", None))
    out_specs = (P("tm", "space", None), P())

    def choose(rhs, guess, diffusion):
        points = rhs.shape[0] * lax.axis_size("tm")
        one_coarsest = points == 2 ** (LEVELS - 1) and rhs.shape[0] == 2
        even = rhs.shape[1] % (TILE * lax.axis_size("tm")) == 0 and rhs.shape[2] % 128 == 0
        if one_coarsest and even:
            return fast_body(rhs, guess, diffusion)
        return body(rhs, guess, diffusion)

    return jax.shard_map(choose, mesh=mesh, in_specs=in_specs, out_specs=out_specs, check_vma=False)
```

```python
import functools

import jax
import jax.numpy as jnp
from jax import lax
from jax.experimental import pallas as pl
from jax.experimental.pallas import tpu as pltpu
from jax.sharding import PartitionSpec as P

LEVELS = 5


damping = 0.8


def with_halo(block, sides, width):
    for axis, dim in sides:
        count = lax.axis_size(axis)
        forward = [(i, i + 1) for i in range(count - 1)]
        backward = [(target, source) for source, target in forward]
        low = lax.ppermute(
            lax.slice_in_dim(block, block.shape[dim] - width, None, axis=dim), axis, forward
        )
        high = lax.ppermute(lax.slice_in_dim(block, 0, width, axis=dim), axis, backward)
        block = jnp.concatenate([low, block, high], axis=dim)
    return block


def shifted(value, axis, steps):
    count = lax.axis_size(axis)
    first, last = (max(0, -steps), min(count, count - steps))
    return lax.ppermute(value, axis, [(source, source + steps) for source in range(first, last)])


def from_partner(value, axis, apart):
    mask = 2**apart
    pairs = [(source, source ^ mask) for source in range(lax.axis_size(axis))]
    return lax.ppermute(value, axis, pairs)


def neighbours(field):
    rows = with_halo(field, (("space", 1),), 1)
    padded = jnp.pad(rows, ((0, 0), (0, 0), (1, 1)))
    total = padded[:, 2:, 1:-1] + padded[:, :-2, 1:-1]
    total = total + padded[:, 1:-1, 2:] + padded[:, 1:-1, :-2]
    return total


def residual(field, source, scaled, diag, stride):
    earlier = shifted(field[-1:], "tm", stride)
    before = jnp.concatenate([earlier, field[:-1]], axis=0)
    image = diag * field - scaled * neighbours(field) - before
    return source - image


def stride_of(level):
    if level == 0:
        return 1
    return 2 ** (level - 1)


def body(rhs, guess, diffusion):
    position = lax.axis_index("tm")
    cells = rhs.shape[1] * lax.axis_size("space") * rhs.shape[2]
    partials = []

    def weight_of(level):
        if level <= 1:
            return jnp.float32(1.0)
        stride = stride_of(level)
        return jnp.where(position % stride == stride - 1, 1.0, 0.0).astype(jnp.float32)

    def record(resid, level):
        local_part = jnp.sum(resid * resid) * weight_of(level)
        partials.append(local_part)

    sources = [rhs]
    fields = []
    field = guess
    for level in range(LEVELS - 1):
        source = sources[level]
        scaled = 2.0**level * diffusion
        diag = 1.0 + 4.0 * scaled
        stride = stride_of(level)
        if level == 0:
            field = field + damping * residual(field, source, scaled, diag, stride) / diag
        else:
            field = damping * source / diag
        resid = residual(field, source, scaled, diag, stride)
        record(resid, level)
        fields.append(field)
        if level == 0:
            coarse = resid[0:1] + resid[1:2]
        else:
            coarse = resid + from_partner(resid, "tm", level - 1)
        sources.append(coarse)
    level = LEVELS - 1
    source = sources[level]
    scaled = 2.0**level * diffusion
    diag = 1.0 + 4.0 * scaled
    stride = stride_of(level)
    field = damping * source / diag
    field = field + damping * residual(field, source, scaled, diag, stride) / diag
    resid = residual(field, source, scaled, diag, stride)
    record(resid, level)
    correction = field
    for level in range(LEVELS - 2, -1, -1):
        scaled = 2.0**level * diffusion
        diag = 1.0 + 4.0 * scaled
        stride = stride_of(level)
        field = fields[level] + correction
        field = field + damping * residual(field, sources[level], scaled, diag, stride) / diag
        correction = field
    scaled = 1.0 * diffusion
    diag = 1.0 + 4.0 * scaled
    resid = residual(correction, rhs, scaled, diag, 1)
    record(resid, 0)
    totals = lax.psum(jnp.stack(partials), ("tm", "space"))
    norms = jnp.sqrt(totals / cells)
    return (correction, norms)


DEVICE = pl.DeviceIdType.MESH
TILE = 8
EDGE = 2 * TILE
BLOCK = 64
EARLY = 3
LANES = 128


def cycle_kernel(
    strips, devices, cells,
    rhs_in, guess_in, diff_in, out, norms_out,
    rhs, guess, diff, v0, v1, v1f, sol, guess_e, v0_e, v1f_e, early, early_e, weights,
    c_weights, c_fields, c_sums, c_top, c_v1f, tile, gathered, gathered_z,
    load_sem, zs_sem, zr_sem, ts_sem, tr_sem, as_sem, ar_sem, al_sem,
    bs_sem, br_sem, bl_sem, rs_sem, ns_sem, nr_sem, ms_sem, mr_sem,
):
    me = lax.axis_index("tm")
    strip = lax.axis_index("space")
    rows, width = rhs_in.shape[1], rhs_in.shape[2]
    tiles = width // LANES
    core = lax.rem(me, 2)
    sibling = me + 1 - 2 * core
    chip = me // 2
    chip_x = chip + 1 - 2 * lax.rem(chip, 2)
    chip_y = lax.rem(chip + 2, 4)
    chip_xy = lax.rem(chip_x + 2, 4)
    low, high = EDGE, EDGE + rows
    first, last = me == 0, me == devices - 1
    top, bottom = strip == 0, strip == strips - 1
    piece = rows // devices
    tall_piece = piece + 2 * TILE

    def aligned(value):
        return pl.multiple_of(value, TILE)

    def tm_copy(src, dst, send, recv, target):
        return pltpu.make_async_remote_copy(
            src_ref=src, dst_ref=dst, send_sem=send, recv_sem=recv,
            device_id={"tm": target, "space": strip}, device_id_type=DEVICE,
        )

    def space_copy(src, dst, send, recv, target):
        return pltpu.make_async_remote_copy(
            src_ref=src, dst_ref=dst, send_sem=send, recv_sem=recv,
            device_id={"tm": me, "space": target}, device_id_type=DEVICE,
        )

    later = jnp.minimum(me + 1, devices - 1)
    inside = slice(low, high)

    def load(index, source, target):
        return [
            pltpu.make_async_copy(
                source.at[:, j * LANES:(j + 1) * LANES], target.at[j, inside], load_sem.at[index, j]
            )
            for j in range(tiles)
        ]

    loads = [
        load(0, guess_in.at[1], guess.at[1]), load(1, guess_in.at[0], guess.at[0]), load(2, diff_in, diff),
        load(3, rhs_in.at[1], rhs.at[1]), load(4, rhs_in.at[0], rhs.at[0]),
    ]
    for group in loads:
        for copy in group:
            copy.start()

    barrier = pltpu.get_barrier_semaphore()
    for i in range(1, devices):
        pl.semaphore_signal(
            barrier, inc=1, device_id={"tm": lax.rem(me + i, devices), "space": strip}, device_id_type=DEVICE
        )
    for i in range(1, strips):
        pl.semaphore_signal(
            barrier, inc=1, device_id={"tm": me, "space": lax.rem(strip + i, strips)}, device_id_type=DEVICE
        )

    def row_tiles(start, size):
        return [start + i * TILE for i in range(size // TILE)]

    def blocks(start, size, step, carry=0):
        count = size // BLOCK

        def run(i, carry):
            begin = aligned(start + i * BLOCK)
            for offset in range(0, BLOCK, TILE):
                carry = step(begin + offset, carry)
            return carry

        if count == 1:
            carry = run(0, carry)
        elif count:
            carry = lax.fori_loop(0, count, run, carry)
        for r in row_tiles(start + count * BLOCK, size - count * BLOCK):
            carry = step(r, carry)
        return carry

    def at(r):
        return pl.ds(r, TILE)

    zero = jnp.zeros((TILE, LANES), jnp.float32)

    @pl.when(first)
    def _():
        def clear(r, carry):
            for ref in (guess_e, v0_e, v1f_e, early_e):
                for j in range(tiles):
                    ref[j, at(r), :] = zero
            return carry

        blocks(low - TILE, rows + 2 * TILE, clear)

    def clear_edge(start):
        for j in range(tiles):
            for ref in (guess, rhs):
                for p in range(2):
                    ref[p, j, start:start + TILE, :] = zero
            for ref in (v1, v1f, guess_e, v0_e, diff):
                ref[j, start:start + TILE, :] = zero

    @pl.when(top)
    def _():
        clear_edge(low - TILE)

    @pl.when(bottom)
    def _():
        clear_edge(high)

    pl.semaphore_wait(barrier, devices + strips - 2)

    down = jnp.minimum(strip + 1, strips - 1)
    up = jnp.maximum(strip - 1, 0)

    def halo_pair(index, field, lead=()):
        def rows_at(start):
            return field.at[lead + (slice(None), slice(start, start + TILE))]

        return (
            space_copy(rows_at(high - TILE), rows_at(low - TILE), zs_sem.at[index, 0], zr_sem.at[index, 0], down),
            space_copy(rows_at(low), rows_at(high), zs_sem.at[index, 1], zr_sem.at[index, 1], up),
        )

    guess_halo = halo_pair(0, guess, (slice(None),))
    diff_halo = halo_pair(1, diff)
    rhs_halo = halo_pair(2, rhs, (slice(None),))
    v1_halo, v1f_halo, guess_e_halo, v0_e_halo = [
        halo_pair(3 + i, field) for i, field in enumerate((v1, v1f, guess_e, v0_e))
    ]

    def start_halo(pair_of):
        @pl.when(jnp.logical_not(bottom))
        def _():
            pair_of[0].start()

        @pl.when(jnp.logical_not(top))
        def _():
            pair_of[1].start()

    def finish_halo(pair_of):
        @pl.when(jnp.logical_not(top))
        def _():
            pair_of[0].wait_recv()
            pair_of[1].wait_send()

        @pl.when(jnp.logical_not(bottom))
        def _():
            pair_of[1].wait_recv()
            pair_of[0].wait_send()

    half = rows // 2
    quarter = rows // 4
    whole = [
        (low - TILE, quarter + TILE), (low + quarter, quarter),
        (low + 2 * quarter, quarter), (low + 3 * quarter, quarter + TILE),
    ]
    inner = [(low + quarter * j, quarter) for j in range(4)]
    guess_parts = [(low, half), (low + half, half)]

    def shift(stage, source, target, parts):
        return [
            tm_copy(
                source.at[:, start:start + size], target.at[:, start:start + size],
                ts_sem.at[stage, j], tr_sem.at[stage, j], later,
            )
            for j, (start, size) in enumerate(parts)
        ]

    def send(copy):
        @pl.when(jnp.logical_not(last))
        def _():
            copy.start()

    def receive(copy):
        @pl.when(jnp.logical_not(first))
        def _():
            copy.wait_recv()

    guess_shift = shift(0, guess.at[1], guess_e, guess_parts)
    v0_shift = shift(1, v0.at[1], v0_e, inner)
    early_shift = shift(2, early, early_e, inner)

    for copy in loads[0]:
        copy.wait()
    send(guess_shift[0])
    send(guess_shift[1])
    for copy in loads[1]:
        copy.wait()
    start_halo(guess_halo)
    for copy in loads[2]:
        copy.wait()
    start_halo(diff_halo)
    for copy in loads[3] + loads[4]:
        copy.wait()
    start_halo(rhs_halo)

    lane = lax.broadcasted_iota(jnp.int32, (TILE, LANES), 1)
    at_left, at_right = lane == 0, lane == LANES - 1

    def stencil(field, r):
        mids = [field[j, at(r), :] for j in range(tiles)]
        right = [zero] + [pltpu.roll(mid, 1, 1) for mid in mids]
        left = [pltpu.roll(mid, LANES - 1, 1) for mid in mids] + [zero]
        totals = []
        for j in range(tiles):
            total = field[j, at(r - 1), :] + field[j, at(r + 1), :]
            total = total + jnp.where(at_left, right[j], right[j + 1])
            totals.append(total + jnp.where(at_right, left[j + 1], left[j]))
        return mids, totals

    def squares(values):
        total = values[0] * values[0]
        for value in values[1:]:
            total = total + value * value
        return total

    keep_share = 1.0 - damping

    def set_weights(r, carry):
        for j in range(tiles):
            scaled = diff[j, at(r), :]
            for level in range(2):
                weights[level, j, at(r), :] = damping / (1.0 + 4.0 * (2.0**level * scaled))
        return carry

    def sweep(p, source, before, target, also=None):
        def step(r, carry):
            mids, totals = stencil(source, r)
            for j in range(tiles):
                inner_sum = rhs[p, j, at(r), :] + diff[j, at(r), :] * totals[j] + before[j, at(r), :]
                value = keep_share * mids[j] + weights[0, j, at(r), :] * inner_sum
                target[j, at(r), :] = value
                if also is not None:
                    also(j, r, value)
            return carry

        return step

    def level_residual(p, j, r, mid, total, before):
        scaled = diff[j, at(r), :]
        return rhs[p, j, at(r), :] - mid + scaled * (total - 4.0 * mid) + before

    sweep_last = sweep(1, guess.at[1], guess.at[0], v0.at[1])
    blocks(low, rows, set_weights)
    blocks(low + quarter, 2 * quarter, sweep_last)
    finish_halo(guess_halo)
    finish_halo(diff_halo)
    finish_halo(rhs_halo)
    set_weights(low - TILE, 0)
    set_weights(high, 0)
    for j in (0, 3):
        blocks(*whole[j], sweep_last)
    for j in (0, 3, 1, 2):
        send(v0_shift[j])

    c_low, c_high = EDGE, EDGE + piece
    c_rows = slice(c_low - TILE, c_high + TILE)
    c_tiles, c_own = row_tiles(c_low - TILE, tall_piece), row_tiles(c_low, piece)
    offset = me * piece

    def coarse_diff(j, r):
        return diff[j, at(aligned(r + offset)), :]

    def coarse_weights(i, carry):
        r = aligned(c_low - TILE + i * TILE)
        for j in range(tiles):
            base = coarse_diff(j, r)
            for level in range(1, LEVELS):
                c_weights[level - 1, j, at(r), :] = damping / (1.0 + 4.0 * (2.0**level * base))
        return carry

    lax.fori_loop(0, tall_piece // TILE, coarse_weights, 0)

    def keep_early(j, r, value):
        early[j, at(r), :] = rhs[1, j, at(r), :] + value

    for copy in guess_shift:
        receive(copy)

    @pl.when(jnp.logical_not(first))
    def _():
        start_halo(guess_e_halo)

    halo_tiles = (low - TILE, high)
    sweep_first = sweep(0, guess.at[0], guess_e, v0.at[0], keep_early)
    blocks(low, rows, sweep_first)

    @pl.when(jnp.logical_not(first))
    def _():
        finish_halo(guess_e_halo)

    for r in halo_tiles:
        sweep_first(r, 0)

    def descend(r, carry):
        firsts, totals = stencil(v0.at[0], r)
        lasts, totals_last = stencil(v0.at[1], r)
        ones, twos = [], []
        for j in range(tiles):
            ones.append(level_residual(0, j, r, firsts[j], totals[j], v0_e[j, at(r), :]))
            twos.append(level_residual(1, j, r, lasts[j], totals_last[j], firsts[j]))
            v1[j, at(r), :] = weights[1, j, at(r), :] * (ones[j] + twos[j])
        return carry + (squares(ones) + squares(twos))

    c_v1 = c_fields[0]

    def row_place(k, ahead=0):
        return aligned(low - ahead + k * piece)

    def hand_over(slot, k):
        source = v1.at[:, pl.ds(row_place(k, TILE), tall_piece)]
        return tm_copy(source, c_v1.at[me, :, c_rows], as_sem.at[slot], ar_sem.at[me], k)

    total0 = zero
    for j in (0, 3, 1, 2):
        receive(v0_shift[j])
        total0 = blocks(*inner[j], descend, total0)
        if j == 3:
            start_halo(v1_halo)
    finish_halo(v1_halo)
    others = [2 * c + i for c in (chip_x, chip_y) for i in range(2)] + [sibling] + [2 * chip_xy, 2 * chip_xy + 1]
    handed = [hand_over(slot, k) for slot, k in enumerate(others)]
    for copy in handed:
        copy.start()
    local = pltpu.make_async_copy(
        v1.at[:, pl.ds(row_place(me, TILE), tall_piece)], c_v1.at[me, :, c_rows], al_sem
    )
    local.start()
    local.wait()
    for copy in early_shift[:EARLY]:
        send(copy)
    for s in range(devices):
        copy = tm_copy(c_v1.at[s, :, c_rows], c_v1.at[s, :, c_rows], as_sem.at[0], ar_sem.at[s], sibling)

        @pl.when(s != me)
        def _():
            copy.wait_recv()

    coarsest = LEVELS - 1

    def coarse_residual(level):
        field, target = c_fields[level - 1], c_fields[level]
        count = devices >> (level - 1)
        carry = zero
        for r in c_tiles:
            own = c_low <= r < c_high
            scaled = [2.0**level * coarse_diff(j, r) for j in range(tiles)]
            earlier, even = None, None
            for p in range(count):
                mids, totals = stencil(field.at[p], r)
                resid = []
                for j in range(tiles):
                    value = 0.25 * mids[j] + scaled[j] * (mids[j] + totals[j])
                    resid.append(value + earlier[j] if p else value)
                earlier = mids
                if own:
                    carry = carry + squares(resid)
                if p % 2 == 0:
                    even = resid
                else:
                    for j in range(tiles):
                        target[p // 2, j, at(r), :] = c_weights[level, j, at(r), :] * (even[j] + resid[j])
        return carry

    def lift(level, p, j, r, value):
        for q in (2 * p, 2 * p + 1):
            c_sums[level - 1][q, j, at(r), :] = c_fields[level - 1][q, j, at(r), :] + value

    def coarse_final(level, p, r, mids, totals, scaled, earlier):
        values = []
        for j in range(tiles):
            value = scaled[j] * totals[j]
            if p:
                value = value + earlier[j]
            value = c_fields[level - 1][p, j, at(r), :] + c_weights[level - 1, j, at(r), :] * value
            values.append(keep_share * mids[j] + value)
        return values

    parts = [total0]
    for level in range(1, coarsest):
        parts.append(coarse_residual(level))

    field_l = c_fields[coarsest - 1].at[0]
    for r in c_tiles:
        mids, totals = stencil(field_l, r)
        for j in range(tiles):
            scaled = 2.0**coarsest * coarse_diff(j, r)
            value = (1.0 + keep_share) * mids[j] + c_weights[coarsest - 1, j, at(r), :] * (scaled * totals[j])
            c_top[j, at(r), :] = value
            lift(coarsest - 1, 0, j, r, value)
    for level in range(coarsest - 1, 1, -1):
        for r in c_tiles:
            scaled = [2.0**level * coarse_diff(j, r) for j in range(tiles)]
            earlier = None
            for p in range(devices >> (level - 1)):
                mids, totals = stencil(c_sums[level - 1].at[p], r)
                values = coarse_final(level, p, r, mids, totals, scaled, earlier)
                earlier = mids
                for j in range(tiles):
                    lift(level - 1, p, j, r, values[j])

    back = []
    place = pl.ds(row_place(me), piece)

    def give_back(kind, slot, target, point):
        src, dst = c_v1f.at[point, :, c_low:c_high], (v1f, v1f_e)[kind].at[:, place]
        return tm_copy(src, dst, bs_sem.at[kind, slot], br_sem.at[kind, me], target)

    def keep_back(kind, point):
        src, dst = c_v1f.at[point, :, c_low:c_high], (v1f, v1f_e)[kind].at[:, place]
        local = pltpu.make_async_copy(src, dst, bl_sem.at[kind])
        local.start()
        local.wait()

    for r in c_own:
        scaled = [2.0 * coarse_diff(j, r) for j in range(tiles)]
        earlier = None
        for p in range(devices):
            mids, totals = stencil(c_sums[0].at[p], r)
            values = coarse_final(1, p, r, mids, totals, scaled, earlier)
            earlier = mids
            for j in range(tiles):
                c_v1f[p, j, at(r), :] = values[j]
    back_own = [give_back(0, slot, k, k) for slot, k in enumerate(others)]
    back_before = [give_back(1, slot, 2 * c, jnp.maximum(2 * c - 1, 0)) for slot, c in enumerate((chip_x, chip_y, chip_xy))]
    to_sibling = give_back(1, 3, sibling, jnp.maximum(sibling - 1, 0))
    has_before = [c > 0 for c in (chip_x, chip_y, chip_xy)]
    inner_chip = jnp.logical_and(core == 1, chip > 0)

    def start_before(i):
        @pl.when(has_before[i])
        def _():
            back_before[i].start()

    for copy in back_own[:4]:
        copy.start()
    start_before(0)
    start_before(1)
    for copy in back_own[5:]:
        copy.start()
    start_before(2)
    back_own[4].start()

    @pl.when(inner_chip)
    def _():
        to_sibling.start()

    keep_back(0, me)

    @pl.when(jnp.logical_and(core == 0, chip > 0))
    def _():
        keep_back(1, jnp.maximum(me - 1, 0))

    for copy in early_shift[EARLY:]:
        send(copy)

    total_l = zero
    for r in c_own:
        mids, totals = stencil(c_top, r)
        resid = []
        for j in range(tiles):
            scaled = 2.0**coarsest * coarse_diff(j, r)
            ahead = (1.0 + keep_share / damping) * field_l[j, at(r), :] - mids[j]
            resid.append((1.0 + 4.0 * scaled) * ahead + scaled * totals[j])
        total_l = total_l + squares(resid)
    parts.append(total_l)

    @pl.when(jnp.logical_not(last))
    def _():
        for copy in v0_shift:
            copy.wait_send()

    def spots_of(field, k):
        return field.at[:, pl.ds(row_place(k), piece)]

    def relay(slot, k):
        return tm_copy(spots_of(v1f, k), spots_of(v1f_e, k), rs_sem.at[slot], br_sem.at[1, k], sibling)

    def absorb(spots):
        for r in spots:
            for j in range(tiles):
                value = v1f[j, at(r), :]
                for p in range(2):
                    v0[p, j, at(r), :] = v0[p, j, at(r), :] + value

    order = [me, sibling] + others[:4] + others[5:]
    relays = [relay(slot, k) for slot, k in enumerate(order)]

    def place_tiles(k):
        return [row_place(k) + i * TILE for i in range(piece // TILE)]

    for slot, k in enumerate(order):
        if slot:
            spots = spots_of(v1f, k)
            tm_copy(spots, spots, rs_sem.at[slot], br_sem.at[0, k], sibling).wait_recv()

        @pl.when(core == 0)
        def _():
            relays[slot].start()

        absorb(place_tiles(k))
    start_halo(v1f_halo)

    def ascend_last(r, carry, store=True):
        mids, totals = stencil(v0.at[1], r)
        for j in range(tiles):
            inner_sum = rhs[1, j, at(r), :] + diff[j, at(r), :] * totals[j] + v0[0, j, at(r), :]
            value = keep_share * mids[j] + weights[0, j, at(r), :] * inner_sum
            sol[1, j, at(r), :] = value
            if store:
                out[1, at(r - low), j * LANES:(j + 1) * LANES] = value
        return carry

    def ascend_first(r, carry):
        mids, totals = stencil(v0.at[0], r)
        for j in range(tiles):
            inner_sum = rhs[0, j, at(r), :] + diff[j, at(r), :] * totals[j]
            sol[0, j, at(r), :] = keep_share * mids[j] + weights[0, j, at(r), :] * inner_sum
        return carry

    blocks(low + TILE, rows - 2 * TILE, ascend_last)
    finish_halo(v1f_halo)
    absorb(halo_tiles)
    for r in (low, high - TILE):
        ascend_last(r, 0)
    for r in halo_tiles:
        ascend_last(r, 0, False)
    blocks(low - TILE, rows + 2 * TILE, ascend_first)

    def final_last(r, carry):
        mids, totals = stencil(sol.at[1], r)
        for j in range(tiles):
            rhs[1, j, at(r), :] = level_residual(1, j, r, mids[j], totals[j], 0.0)
        return carry

    blocks(low, rows, final_last)

    def complete(r, carry):
        resid = []
        for j in range(tiles):
            before = v0_e[j, at(r), :] + v1f_e[j, at(r), :]
            v0_e[j, at(r), :] = before
            value = sol[0, j, at(r), :] + weights[0, j, at(r), :] * before
            sol[0, j, at(r), :] = value
            out[0, at(r - low), j * LANES:(j + 1) * LANES] = value
            resid.append(rhs[1, j, at(r), :] + value)
        return carry + squares(resid)

    total5 = zero
    for slot, k in enumerate(order):
        @pl.when(jnp.logical_or(core == 1, chip > 0) if slot else core == 1)
        def _():
            relays[slot].wait_recv()

        for r in place_tiles(k):
            total5 = complete(r, total5)

    @pl.when(jnp.logical_not(first))
    def _():
        start_halo(v0_e_halo)

    def final_first(r, carry):
        mids, totals = stencil(v0_e, r)
        befores = []
        for j in range(tiles):
            inner_sum = early_e[j, at(r), :] + v1f_e[j, at(r), :] + diff[j, at(r), :] * totals[j]
            befores.append(keep_share * mids[j] + weights[0, j, at(r), :] * inner_sum)
        mids, totals = stencil(sol.at[0], r)
        return carry + squares([
            level_residual(0, j, r, mids[j], totals[j], befores[j]) for j in range(tiles)
        ])

    for copy in early_shift:
        receive(copy)
    total5 = blocks(low + TILE, rows - 2 * TILE, final_first, total5)

    @pl.when(jnp.logical_not(first))
    def _():
        finish_halo(v0_e_halo)

    for r in halo_tiles:
        for j in range(tiles):
            sol[0, j, at(r), :] = sol[0, j, at(r), :] + weights[0, j, at(r), :] * v0_e[j, at(r), :]
    for r in (low, high - TILE):
        total5 = final_first(r, total5)

    parts.append(total5)
    for level, value in enumerate(parts):
        tile[level:level + 1, :] = jnp.sum(value, axis=0, keepdims=True)
    for level in range(len(parts), TILE):
        tile[level:level + 1, :] = jnp.zeros((1, LANES), jnp.float32)

    def exchange(count, own, source, slots, copier, send_sems, recv_sems):
        slots[pl.ds(own, 1)] = source[...][None]
        sent = [
            copier(source, slots.at[own], send_sems.at[i], recv_sems.at[own], lax.rem(own + i, count))
            for i in range(1, count)
        ]
        for copy in sent:
            copy.start()
        for i in range(1, count):
            other = lax.rem(own + i, count)
            copier(source, slots.at[other], send_sems.at[i], recv_sems.at[other], other).wait_recv()
        for copy in sent:
            copy.wait_send()
        total = slots[0]
        for i in range(1, count):
            total = total + slots[i]
        return total

    total = exchange(devices, me, tile, gathered, tm_copy, ns_sem, nr_sem)
    tile[...] = total
    total = exchange(strips, strip, tile, gathered_z, space_copy, ms_sem, mr_sem)
    summed = jnp.sum(total, axis=1, keepdims=True)
    norms_out[...] = jnp.broadcast_to(jnp.sqrt(summed * (1.0 / cells)), (TILE, LANES))

    @pl.when(jnp.logical_not(last))
    def _():
        for copy in guess_shift + early_shift:
            copy.wait_send()

    for copy in handed + back_own:
        copy.wait_send()
    for i in range(3):
        @pl.when(has_before[i])
        def _():
            back_before[i].wait_send()

    @pl.when(inner_chip)
    def _():
        to_sibling.wait_send()

    @pl.when(core == 0)
    def _():
        for copy in relays:
            copy.wait_send()


def fast_body(rhs, guess, diffusion):
    devices, strips = lax.axis_size("tm"), lax.axis_size("space")
    rows, width = rhs.shape[1:]
    tiles = width // LANES
    cells = rows * strips * width

    def spread(height):
        return height + (TILE - height) % (4 * TILE)

    def plane(*lead):
        return pltpu.VMEM(lead + (tiles, spread(rows + 2 * EDGE), LANES), jnp.float32)

    def coarse(*lead):
        return pltpu.VMEM(lead + (tiles, spread(rows // devices + 2 * EDGE), LANES), jnp.float32)

    dma = pltpu.SemaphoreType.DMA
    scratch = [
        plane(2), plane(2), plane(), plane(2), plane(), plane(), plane(2),
        plane(), plane(), plane(), plane(), plane(), plane(2),
        coarse(LEVELS - 1), tuple(coarse(devices >> level) for level in range(LEVELS - 1)),
        tuple(coarse(devices >> level) for level in range(LEVELS - 2)), coarse(), coarse(devices),
        pltpu.VMEM((TILE, LANES), jnp.float32),
        pltpu.VMEM((devices, TILE, LANES), jnp.float32),
        pltpu.VMEM((strips, TILE, LANES), jnp.float32),
        dma((5, tiles)), dma((7, 2)), dma((7, 2)), dma((3, 4)), dma((3, 4)), dma((devices,)), dma((devices,)), dma,
        dma((2, devices)), dma((2, devices)), dma((2,)), dma((devices,)),
        dma((devices,)), dma((devices,)), dma((strips,)), dma((strips,)),
    ]
    any_space = pl.BlockSpec(memory_space=pl.ANY)
    result, norms = pl.pallas_call(
        functools.partial(cycle_kernel, strips, devices, cells),
        out_shape=(
            pltpu.VMEM(rhs.shape, jnp.float32),
            jax.ShapeDtypeStruct((TILE, LANES), jnp.float32),
        ),
        in_specs=[any_space] * 3,
        out_specs=(pl.BlockSpec(memory_space=pltpu.VMEM), pl.BlockSpec(memory_space=pltpu.VMEM)),
        scratch_shapes=scratch,
        compiler_params=pltpu.CompilerParams(
            collective_id=0, has_side_effects=True, vmem_limit_bytes=67_043_328 - rhs.size * 4 - 2**17
        ),
    )(rhs, guess, diffusion)
    return result, norms[:LEVELS + 1, 0]


def solution(mesh):
    in_specs = (P("tm", "space", None), P("tm", "space", None), P("space", None))
    out_specs = (P("tm", "space", None), P())

    def choose(rhs, guess, diffusion):
        points = rhs.shape[0] * lax.axis_size("tm")
        one_coarsest = points == 2 ** (LEVELS - 1) and rhs.shape[0] == 2
        even = rhs.shape[1] % (TILE * lax.axis_size("tm")) == 0 and rhs.shape[2] % 128 == 0
        if one_coarsest and even:
            return fast_body(rhs, guess, diffusion)
        return body(rhs, guess, diffusion)

    return jax.shard_map(choose, mesh=mesh, in_specs=in_specs, out_specs=out_specs, check_vma=False)
```

```python
import functools

import jax
import jax.numpy as jnp
from jax import lax
from jax.experimental import pallas as pl
from jax.experimental.pallas import tpu as pltpu
from jax.sharding import PartitionSpec as P

LEVELS = 5


damping = 0.8


def with_halo(block, sides, width):
    for axis, dim in sides:
        count = lax.axis_size(axis)
        forward = [(i, i + 1) for i in range(count - 1)]
        backward = [(target, source) for source, target in forward]
        low = lax.ppermute(
            lax.slice_in_dim(block, block.shape[dim] - width, None, axis=dim), axis, forward
        )
        high = lax.ppermute(lax.slice_in_dim(block, 0, width, axis=dim), axis, backward)
        block = jnp.concatenate([low, block, high], axis=dim)
    return block


def shifted(value, axis, steps):
    count = lax.axis_size(axis)
    first, last = (max(0, -steps), min(count, count - steps))
    return lax.ppermute(value, axis, [(source, source + steps) for source in range(first, last)])


def from_partner(value, axis, apart):
    mask = 2**apart
    pairs = [(source, source ^ mask) for source in range(lax.axis_size(axis))]
    return lax.ppermute(value, axis, pairs)


def neighbours(field):
    rows = with_halo(field, (("space", 1),), 1)
    padded = jnp.pad(rows, ((0, 0), (0, 0), (1, 1)))
    total = padded[:, 2:, 1:-1] + padded[:, :-2, 1:-1]
    total = total + padded[:, 1:-1, 2:] + padded[:, 1:-1, :-2]
    return total


def residual(field, source, scaled, diag, stride):
    earlier = shifted(field[-1:], "tm", stride)
    before = jnp.concatenate([earlier, field[:-1]], axis=0)
    image = diag * field - scaled * neighbours(field) - before
    return source - image


def stride_of(level):
    if level == 0:
        return 1
    return 2 ** (level - 1)


def body(rhs, guess, diffusion):
    position = lax.axis_index("tm")
    cells = rhs.shape[1] * lax.axis_size("space") * rhs.shape[2]
    partials = []

    def weight_of(level):
        if level <= 1:
            return jnp.float32(1.0)
        stride = stride_of(level)
        return jnp.where(position % stride == stride - 1, 1.0, 0.0).astype(jnp.float32)

    def record(resid, level):
        local_part = jnp.sum(resid * resid) * weight_of(level)
        partials.append(local_part)

    sources = [rhs]
    fields = []
    field = guess
    for level in range(LEVELS - 1):
        source = sources[level]
        scaled = 2.0**level * diffusion
        diag = 1.0 + 4.0 * scaled
        stride = stride_of(level)
        if level == 0:
            field = field + damping * residual(field, source, scaled, diag, stride) / diag
        else:
            field = damping * source / diag
        resid = residual(field, source, scaled, diag, stride)
        record(resid, level)
        fields.append(field)
        if level == 0:
            coarse = resid[0:1] + resid[1:2]
        else:
            coarse = resid + from_partner(resid, "tm", level - 1)
        sources.append(coarse)
    level = LEVELS - 1
    source = sources[level]
    scaled = 2.0**level * diffusion
    diag = 1.0 + 4.0 * scaled
    stride = stride_of(level)
    field = damping * source / diag
    field = field + damping * residual(field, source, scaled, diag, stride) / diag
    resid = residual(field, source, scaled, diag, stride)
    record(resid, level)
    correction = field
    for level in range(LEVELS - 2, -1, -1):
        scaled = 2.0**level * diffusion
        diag = 1.0 + 4.0 * scaled
        stride = stride_of(level)
        field = fields[level] + correction
        field = field + damping * residual(field, sources[level], scaled, diag, stride) / diag
        correction = field
    scaled = 1.0 * diffusion
    diag = 1.0 + 4.0 * scaled
    resid = residual(correction, rhs, scaled, diag, 1)
    record(resid, 0)
    totals = lax.psum(jnp.stack(partials), ("tm", "space"))
    norms = jnp.sqrt(totals / cells)
    return (correction, norms)


DEVICE = pl.DeviceIdType.MESH
TILE = 8
EDGE = 2 * TILE
BLOCK = 64
EARLY = 2
LANES = 128


def cycle_kernel(
    strips, devices, cells,
    rhs_in, guess_in, diff_in, out, norms_out,
    rhs, guess, diff, v0, v1, v1f, sol, guess_e, v0_e, v1f_e, early, early_e, weights,
    c_weights, c_fields, c_sums, c_top, c_v1f, tile, gathered, gathered_z, final_row, final_rows,
    load_sem, zs_sem, zr_sem, ts_sem, tr_sem, as_sem, ar_sem, al_sem,
    hs_sem, hr_sem, bs_sem, br_sem, bl_sem, rs_sem, ns_sem, nr_sem, ms_sem, mr_sem, fs_sem, fr_sem,
):
    me = lax.axis_index("tm")
    strip = lax.axis_index("space")
    rows, width = rhs_in.shape[1], rhs_in.shape[2]
    tiles = width // LANES
    core = lax.rem(me, 2)
    sibling = me + 1 - 2 * core
    chip = me // 2
    chip_x = chip + 1 - 2 * lax.rem(chip, 2)
    chip_y = lax.rem(chip + 2, 4)
    chip_xy = lax.rem(chip_x + 2, 4)
    low, high = EDGE, EDGE + rows
    first, last = me == 0, me == devices - 1
    top, bottom = strip == 0, strip == strips - 1
    piece = rows // devices
    tall_piece = piece + 2 * TILE

    def aligned(value):
        return pl.multiple_of(value, TILE)

    def tm_copy(src, dst, send, recv, target):
        return pltpu.make_async_remote_copy(
            src_ref=src, dst_ref=dst, send_sem=send, recv_sem=recv,
            device_id={"tm": target, "space": strip}, device_id_type=DEVICE,
        )

    def space_copy(src, dst, send, recv, target):
        return pltpu.make_async_remote_copy(
            src_ref=src, dst_ref=dst, send_sem=send, recv_sem=recv,
            device_id={"tm": me, "space": target}, device_id_type=DEVICE,
        )

    later = jnp.minimum(me + 1, devices - 1)
    inside = slice(low, high)

    def load(index, source, target):
        return [
            pltpu.make_async_copy(
                source.at[:, j * LANES:(j + 1) * LANES], target.at[j, inside], load_sem.at[index, j]
            )
            for j in range(tiles)
        ]

    loads = [
        load(0, guess_in.at[1], guess.at[1]), load(1, guess_in.at[0], guess.at[0]), load(2, diff_in, diff),
        load(3, rhs_in.at[1], rhs.at[1]), load(4, rhs_in.at[0], rhs.at[0]),
    ]
    for group in loads:
        for copy in group:
            copy.start()

    barrier = pltpu.get_barrier_semaphore()
    for i in range(1, devices):
        pl.semaphore_signal(
            barrier, inc=1, device_id={"tm": lax.rem(me + i, devices), "space": strip}, device_id_type=DEVICE
        )
    down = jnp.minimum(strip + 1, strips - 1)
    up = jnp.maximum(strip - 1, 0)
    for edge, beside in ((top, up), (bottom, down)):
        @pl.when(jnp.logical_not(edge))
        def _():
            pl.semaphore_signal(barrier, inc=1, device_id={"tm": me, "space": beside}, device_id_type=DEVICE)

    def row_tiles(start, size):
        return [start + i * TILE for i in range(size // TILE)]

    def blocks(start, size, step, carry=0):
        count = size // BLOCK

        def run(i, carry):
            begin = aligned(start + i * BLOCK)
            for offset in range(0, BLOCK, TILE):
                carry = step(begin + offset, carry)
            return carry

        if count == 1:
            carry = run(0, carry)
        elif count:
            carry = lax.fori_loop(0, count, run, carry)
        for r in row_tiles(start + count * BLOCK, size - count * BLOCK):
            carry = step(r, carry)
        return carry

    def at(r):
        return pl.ds(r, TILE)

    zero = jnp.zeros((TILE, LANES), jnp.float32)

    @pl.when(first)
    def _():
        def clear(r, carry):
            for ref in (guess_e, v0_e, v1f_e, early_e):
                for j in range(tiles):
                    ref[j, at(r), :] = zero
            return carry

        blocks(low - TILE, rows + 2 * TILE, clear)

    def clear_edge(start):
        for j in range(tiles):
            for ref in (guess, rhs):
                for p in range(2):
                    ref[p, j, start:start + TILE, :] = zero
            for ref in (v1, v1f, guess_e, v0_e, diff):
                ref[j, start:start + TILE, :] = zero

    @pl.when(top)
    def _():
        clear_edge(low - TILE)

    @pl.when(bottom)
    def _():
        clear_edge(high)

    pl.semaphore_wait(barrier, devices + 1 - top.astype(jnp.int32) - bottom.astype(jnp.int32))

    def halo_pair(index, field, lead=()):
        def rows_at(start):
            return field.at[lead + (slice(None), slice(start, start + TILE))]

        return (
            space_copy(rows_at(high - TILE), rows_at(low - TILE), zs_sem.at[index, 0], zr_sem.at[index, 0], down),
            space_copy(rows_at(low), rows_at(high), zs_sem.at[index, 1], zr_sem.at[index, 1], up),
        )

    guess_halo = halo_pair(0, guess, (slice(None),))
    diff_halo = halo_pair(1, diff)
    rhs_halo = halo_pair(2, rhs, (slice(None),))
    v1_halo, v1f_halo, guess_e_halo, v0_e_halo = [
        halo_pair(3 + i, field) for i, field in enumerate((v1, v1f, guess_e, v0_e))
    ]

    def start_halo(pair_of):
        @pl.when(jnp.logical_not(bottom))
        def _():
            pair_of[0].start()

        @pl.when(jnp.logical_not(top))
        def _():
            pair_of[1].start()

    def finish_halo(pair_of):
        @pl.when(jnp.logical_not(top))
        def _():
            pair_of[0].wait_recv()
            pair_of[1].wait_send()

        @pl.when(jnp.logical_not(bottom))
        def _():
            pair_of[1].wait_recv()
            pair_of[0].wait_send()

    half = rows // 2
    quarter = rows // 4
    whole = [
        (low - TILE, quarter + TILE), (low + quarter, quarter),
        (low + 2 * quarter, quarter), (low + 3 * quarter, quarter + TILE),
    ]
    inner = [(low + quarter * j, quarter) for j in range(4)]
    guess_parts = [(low, half), (low + half, half)]

    def shift(stage, source, target, parts):
        return [
            tm_copy(
                source.at[:, start:start + size], target.at[:, start:start + size],
                ts_sem.at[stage, j], tr_sem.at[stage, j], later,
            )
            for j, (start, size) in enumerate(parts)
        ]

    def send(copy):
        @pl.when(jnp.logical_not(last))
        def _():
            copy.start()

    def receive(copy):
        @pl.when(jnp.logical_not(first))
        def _():
            copy.wait_recv()

    guess_shift = shift(0, guess.at[1], guess_e, guess_parts)
    v0_shift = shift(1, v0.at[1], v0_e, inner)
    early_shift = shift(2, early, early_e, inner)

    for copy in loads[0]:
        copy.wait()
    send(guess_shift[0])
    send(guess_shift[1])
    for copy in loads[1]:
        copy.wait()
    start_halo(guess_halo)
    for copy in loads[2]:
        copy.wait()
    start_halo(diff_halo)
    for copy in loads[3] + loads[4]:
        copy.wait()
    start_halo(rhs_halo)

    lane = lax.broadcasted_iota(jnp.int32, (TILE, LANES), 1)
    at_left, at_right = lane == 0, lane == LANES - 1

    def stencil(field, r):
        mids = [field[j, at(r), :] for j in range(tiles)]
        right = [zero] + [pltpu.roll(mid, 1, 1) for mid in mids]
        left = [pltpu.roll(mid, LANES - 1, 1) for mid in mids] + [zero]
        totals = []
        for j in range(tiles):
            total = field[j, at(r - 1), :] + field[j, at(r + 1), :]
            total = total + jnp.where(at_left, right[j], right[j + 1])
            totals.append(total + jnp.where(at_right, left[j + 1], left[j]))
        return mids, totals

    def squares(values):
        total = values[0] * values[0]
        for value in values[1:]:
            total = total + value * value
        return total

    keep_share = 1.0 - damping

    def set_weights(r, carry):
        for j in range(tiles):
            scaled = diff[j, at(r), :]
            for level in range(2):
                weights[level, j, at(r), :] = damping / (1.0 + 4.0 * (2.0**level * scaled))
        return carry

    def sweep(p, source, before, target, also=None):
        def step(r, carry):
            mids, totals = stencil(source, r)
            for j in range(tiles):
                inner_sum = rhs[p, j, at(r), :] + diff[j, at(r), :] * totals[j] + before[j, at(r), :]
                value = keep_share * mids[j] + weights[0, j, at(r), :] * inner_sum
                target[j, at(r), :] = value
                if also is not None:
                    also(j, r, value)
            return carry

        return step

    def level_residual(p, j, r, mid, total, before):
        scaled = diff[j, at(r), :]
        return rhs[p, j, at(r), :] - mid + scaled * (total - 4.0 * mid) + before

    sweep_last = sweep(1, guess.at[1], guess.at[0], v0.at[1])
    blocks(low, rows, set_weights)
    blocks(low + quarter, 2 * quarter, sweep_last)
    finish_halo(guess_halo)
    finish_halo(diff_halo)
    finish_halo(rhs_halo)
    set_weights(low - TILE, 0)
    set_weights(high, 0)
    for j in (0, 3):
        blocks(*whole[j], sweep_last)
    for j in (0, 3, 1, 2):
        send(v0_shift[j])

    c_low, c_high = EDGE, EDGE + piece
    c_rows = slice(c_low - TILE, c_high + TILE)
    c_tiles, c_own = row_tiles(c_low - TILE, tall_piece), row_tiles(c_low, piece)
    offset = me * piece

    def coarse_diff(j, r):
        return diff[j, at(aligned(r + offset)), :]

    def coarse_weights(i, carry):
        r = aligned(c_low - TILE + i * TILE)
        for j in range(tiles):
            base = coarse_diff(j, r)
            for level in range(1, LEVELS):
                c_weights[level - 1, j, at(r), :] = damping / (1.0 + 4.0 * (2.0**level * base))
        return carry

    lax.fori_loop(0, tall_piece // TILE, coarse_weights, 0)

    def keep_early(j, r, value):
        early[j, at(r), :] = rhs[1, j, at(r), :] + value

    for copy in guess_shift:
        receive(copy)

    @pl.when(jnp.logical_not(first))
    def _():
        start_halo(guess_e_halo)

    halo_tiles = (low - TILE, high)
    sweep_first = sweep(0, guess.at[0], guess_e, v0.at[0], keep_early)
    blocks(low, rows, sweep_first)

    @pl.when(jnp.logical_not(first))
    def _():
        finish_halo(guess_e_halo)

    for r in halo_tiles:
        sweep_first(r, 0)

    def descend(r, carry):
        firsts, totals = stencil(v0.at[0], r)
        lasts, totals_last = stencil(v0.at[1], r)
        ones, twos = [], []
        for j in range(tiles):
            ones.append(level_residual(0, j, r, firsts[j], totals[j], v0_e[j, at(r), :]))
            twos.append(level_residual(1, j, r, lasts[j], totals_last[j], firsts[j]))
            v1[j, at(r), :] = weights[1, j, at(r), :] * (ones[j] + twos[j])
        return carry + (squares(ones) + squares(twos))

    c_v1 = c_fields[0]

    def row_place(k, ahead=0):
        return aligned(low - ahead + k * piece)

    def hand_over(slot, k, side):
        ahead, size = TILE * (1 - side), piece + TILE
        return tm_copy(
            v1.at[:, pl.ds(row_place(k, ahead), size)],
            c_v1.at[me, :, pl.ds(aligned(c_low - ahead), size)],
            as_sem.at[slot], ar_sem.at[me], k,
        )

    total0 = zero
    for j in (0, 3, 1, 2):
        receive(v0_shift[j])
        total0 = blocks(*inner[j], descend, total0)
        if j == 3:
            start_halo(v1_halo)
    finish_halo(v1_halo)
    others = [2 * c + i for c in (chip_x, chip_y) for i in range(2)] + [sibling] + [2 * chip_xy, 2 * chip_xy + 1]
    far = others[:4] + others[5:]
    tall_here = v1.at[:, pl.ds(row_place(me, TILE), tall_piece)]
    tall_there = v1.at[:, pl.ds(row_place(sibling, TILE), tall_piece)]
    handed = [hand_over(slot, k, slot % 2) for slot, k in enumerate(far)]
    handed.insert(4, tm_copy(tall_there, c_v1.at[me, :, c_rows], as_sem.at[6], ar_sem.at[me], sibling))
    for copy in handed:
        copy.start()
    local = pltpu.make_async_copy(tall_here, c_v1.at[me, :, c_rows], al_sem)
    local.start()
    local.wait()
    for copy in early_shift[:EARLY]:
        send(copy)
    mine = pl.ds(aligned(c_low - TILE * (1 - core)), piece + TILE)
    inner_edge = pl.ds(aligned(c_low + (1 - core) * (piece - TILE)), TILE)
    outer_edge = pl.ds(aligned(c_low - TILE + core * (piece + TILE)), TILE)
    swaps = [
        tm_copy(c_v1.at[k, :, inner_edge], c_v1.at[k, :, outer_edge], hs_sem.at[slot], hr_sem.at[k], sibling)
        for slot, k in enumerate(far)
    ]
    for swap, k in zip(swaps, far):
        spot = c_v1.at[k, :, mine]
        tm_copy(spot, spot, hs_sem.at[0], ar_sem.at[k], sibling).wait_recv()
        swap.start()
    spot = c_v1.at[sibling, :, c_rows]
    tm_copy(spot, spot, hs_sem.at[0], ar_sem.at[sibling], sibling).wait_recv()
    for swap in swaps:
        swap.wait_recv()

    coarsest = LEVELS - 1

    def coarse_residual(level):
        field, target = c_fields[level - 1], c_fields[level]
        count = devices >> (level - 1)
        carry = zero
        for r in c_tiles:
            own = c_low <= r < c_high
            scaled = [2.0**level * coarse_diff(j, r) for j in range(tiles)]
            earlier, even = None, None
            for p in range(count):
                mids, totals = stencil(field.at[p], r)
                resid = []
                for j in range(tiles):
                    value = 0.25 * mids[j] + scaled[j] * (mids[j] + totals[j])
                    resid.append(value + earlier[j] if p else value)
                earlier = mids
                if own:
                    carry = carry + squares(resid)
                if p % 2 == 0:
                    even = resid
                else:
                    for j in range(tiles):
                        target[p // 2, j, at(r), :] = c_weights[level, j, at(r), :] * (even[j] + resid[j])
        return carry

    def lift(level, p, j, r, value):
        for q in (2 * p, 2 * p + 1):
            c_sums[level - 1][q, j, at(r), :] = c_fields[level - 1][q, j, at(r), :] + value

    def coarse_final(level, p, r, mids, totals, scaled, earlier):
        values = []
        for j in range(tiles):
            value = scaled[j] * totals[j]
            if p:
                value = value + earlier[j]
            value = c_fields[level - 1][p, j, at(r), :] + c_weights[level - 1, j, at(r), :] * value
            values.append(keep_share * mids[j] + value)
        return values

    parts = [total0]
    for level in range(1, coarsest):
        parts.append(coarse_residual(level))

    field_l = c_fields[coarsest - 1].at[0]
    for r in c_tiles:
        mids, totals = stencil(field_l, r)
        for j in range(tiles):
            scaled = 2.0**coarsest * coarse_diff(j, r)
            value = (1.0 + keep_share) * mids[j] + c_weights[coarsest - 1, j, at(r), :] * (scaled * totals[j])
            c_top[j, at(r), :] = value
            lift(coarsest - 1, 0, j, r, value)
    for level in range(coarsest - 1, 1, -1):
        for r in c_tiles:
            scaled = [2.0**level * coarse_diff(j, r) for j in range(tiles)]
            earlier = None
            for p in range(devices >> (level - 1)):
                mids, totals = stencil(c_sums[level - 1].at[p], r)
                values = coarse_final(level, p, r, mids, totals, scaled, earlier)
                earlier = mids
                for j in range(tiles):
                    lift(level - 1, p, j, r, values[j])

    total_l = zero
    for r in c_own:
        mids, totals = stencil(c_top, r)
        resid = []
        for j in range(tiles):
            scaled = 2.0**coarsest * coarse_diff(j, r)
            ahead = (1.0 + keep_share / damping) * field_l[j, at(r), :] - mids[j]
            resid.append((1.0 + 4.0 * scaled) * ahead + scaled * totals[j])
        total_l = total_l + squares(resid)
    parts.append(total_l)
    tile[...] = jnp.zeros((TILE, LANES), jnp.float32)
    for level, value in enumerate(parts):
        tile[level:level + 1, :] = jnp.sum(value, axis=0, keepdims=True)

    def begin_sum(count, own, slots, copier, send_sems, recv_sems):
        slots[pl.ds(own, 1)] = tile[...][None]
        sent = [
            copier(tile, slots.at[own], send_sems.at[i], recv_sems.at[own], lax.rem(own + i, count))
            for i in range(1, count)
        ]
        for copy in sent:
            copy.start()

        def end_sum():
            for i in range(1, count):
                other = lax.rem(own + i, count)
                copier(tile, slots.at[other], send_sems.at[i], recv_sems.at[other], other).wait_recv()
            for copy in sent:
                copy.wait_send()
            total = slots[0]
            for i in range(1, count):
                total = total + slots[i]
            tile[...] = total

        return end_sum

    end_time_sum = begin_sum(devices, me, gathered, tm_copy, ns_sem, nr_sem)

    place = pl.ds(row_place(me), piece)

    def give_back(kind, slot, target, point):
        src, dst = c_v1f.at[point, :, c_low:c_high], (v1f, v1f_e)[kind].at[:, place]
        return tm_copy(src, dst, bs_sem.at[kind, slot], br_sem.at[kind, me], target)

    def keep_back(kind, point):
        src, dst = c_v1f.at[point, :, c_low:c_high], (v1f, v1f_e)[kind].at[:, place]
        local = pltpu.make_async_copy(src, dst, bl_sem.at[kind])
        local.start()
        local.wait()

    for r in c_own:
        scaled = [2.0 * coarse_diff(j, r) for j in range(tiles)]
        earlier = None
        for p in range(devices):
            mids, totals = stencil(c_sums[0].at[p], r)
            values = coarse_final(1, p, r, mids, totals, scaled, earlier)
            earlier = mids
            for j in range(tiles):
                c_v1f[p, j, at(r), :] = values[j]
    back_own = [give_back(0, slot, k, k) for slot, k in enumerate(others)]
    back_before = [give_back(1, slot, 2 * c, jnp.maximum(2 * c - 1, 0)) for slot, c in enumerate((chip_x, chip_y, chip_xy))]
    to_sibling = give_back(1, 3, sibling, jnp.maximum(sibling - 1, 0))
    has_before = [c > 0 for c in (chip_x, chip_y, chip_xy)]
    inner_chip = jnp.logical_and(core == 1, chip > 0)

    def start_before(i):
        @pl.when(has_before[i])
        def _():
            back_before[i].start()

    for copy in back_own[:4]:
        copy.start()
    start_before(0)
    start_before(1)
    for copy in back_own[5:]:
        copy.start()
    start_before(2)
    back_own[4].start()

    @pl.when(inner_chip)
    def _():
        to_sibling.start()

    keep_back(0, me)

    @pl.when(jnp.logical_and(core == 0, chip > 0))
    def _():
        keep_back(1, jnp.maximum(me - 1, 0))

    for copy in early_shift[EARLY:]:
        send(copy)

    @pl.when(jnp.logical_not(last))
    def _():
        for copy in v0_shift:
            copy.wait_send()

    def spots_of(field, k):
        return field.at[:, pl.ds(row_place(k), piece)]

    def relay(slot, k):
        return tm_copy(spots_of(v1f, k), spots_of(v1f_e, k), rs_sem.at[slot], br_sem.at[1, k], sibling)

    def absorb(spots):
        for r in spots:
            for j in range(tiles):
                value = v1f[j, at(r), :]
                for p in range(2):
                    v0[p, j, at(r), :] = v0[p, j, at(r), :] + value

    order = [me, sibling] + others[:4] + others[5:]
    relays = [relay(slot, k) for slot, k in enumerate(order)]

    def place_tiles(k):
        return [row_place(k) + i * TILE for i in range(piece // TILE)]

    for slot, k in enumerate(order):
        if slot:
            spots = spots_of(v1f, k)
            tm_copy(spots, spots, rs_sem.at[slot], br_sem.at[0, k], sibling).wait_recv()

        @pl.when(core == 0)
        def _():
            relays[slot].start()

        absorb(place_tiles(k))
    start_halo(v1f_halo)
    end_time_sum()
    end_strip_sum = begin_sum(strips, strip, gathered_z, space_copy, ms_sem, mr_sem)

    def ascend_last(r, carry, store=True):
        mids, totals = stencil(v0.at[1], r)
        for j in range(tiles):
            inner_sum = rhs[1, j, at(r), :] + diff[j, at(r), :] * totals[j] + v0[0, j, at(r), :]
            value = keep_share * mids[j] + weights[0, j, at(r), :] * inner_sum
            sol[1, j, at(r), :] = value
            if store:
                out[1, at(r - low), j * LANES:(j + 1) * LANES] = value
        return carry

    def ascend_first(r, carry):
        mids, totals = stencil(v0.at[0], r)
        for j in range(tiles):
            inner_sum = rhs[0, j, at(r), :] + diff[j, at(r), :] * totals[j]
            sol[0, j, at(r), :] = keep_share * mids[j] + weights[0, j, at(r), :] * inner_sum
        return carry

    blocks(low + TILE, rows - 2 * TILE, ascend_last)
    finish_halo(v1f_halo)
    absorb(halo_tiles)
    for r in (low, high - TILE):
        ascend_last(r, 0)
    for r in halo_tiles:
        ascend_last(r, 0, False)
    blocks(low - TILE, rows + 2 * TILE, ascend_first)

    def final_last(r, carry):
        mids, totals = stencil(sol.at[1], r)
        for j in range(tiles):
            rhs[1, j, at(r), :] = level_residual(1, j, r, mids[j], totals[j], 0.0)
        return carry

    blocks(low, rows, final_last)
    def complete(r, carry):
        resid = []
        for j in range(tiles):
            before = v0_e[j, at(r), :] + v1f_e[j, at(r), :]
            v0_e[j, at(r), :] = before
            value = sol[0, j, at(r), :] + weights[0, j, at(r), :] * before
            sol[0, j, at(r), :] = value
            out[0, at(r - low), j * LANES:(j + 1) * LANES] = value
            resid.append(rhs[1, j, at(r), :] + value)
        return carry + squares(resid)

    total5 = zero
    for slot, k in enumerate(order):
        @pl.when(jnp.logical_or(core == 1, chip > 0) if slot else core == 1)
        def _():
            relays[slot].wait_recv()

        for r in place_tiles(k):
            total5 = complete(r, total5)

    @pl.when(jnp.logical_not(first))
    def _():
        start_halo(v0_e_halo)

    def final_first(r, carry):
        mids, totals = stencil(v0_e, r)
        befores = []
        for j in range(tiles):
            inner_sum = early_e[j, at(r), :] + v1f_e[j, at(r), :] + diff[j, at(r), :] * totals[j]
            befores.append(keep_share * mids[j] + weights[0, j, at(r), :] * inner_sum)
        mids, totals = stencil(sol.at[0], r)
        return carry + squares([
            level_residual(0, j, r, mids[j], totals[j], befores[j]) for j in range(tiles)
        ])

    for i, copy in enumerate(early_shift):
        receive(copy)
        begin, size = inner[i]
        cut_low, cut_high = TILE * (i == 0), TILE * (i == 3)
        total5 = blocks(begin + cut_low, size - cut_low - cut_high, final_first, total5)

    @pl.when(jnp.logical_not(first))
    def _():
        finish_halo(v0_e_halo)

    for r in halo_tiles:
        for j in range(tiles):
            sol[0, j, at(r), :] = sol[0, j, at(r), :] + weights[0, j, at(r), :] * v0_e[j, at(r), :]
    for r in (low, high - TILE):
        total5 = final_first(r, total5)

    final_row[...] = jnp.sum(total5, axis=0, keepdims=True)

    def final_slot(t, z):
        return t * strips + z

    own_slot = final_slot(me, strip)
    final_sent = []
    for i in range(1, devices * strips):
        t, z = lax.rem(me + i // strips, devices), lax.rem(strip + i % strips, strips)
        final_sent.append(pltpu.make_async_remote_copy(
            src_ref=final_row, dst_ref=final_rows.at[own_slot], send_sem=fs_sem.at[i], recv_sem=fr_sem.at[own_slot],
            device_id={"tm": t, "space": z}, device_id_type=DEVICE,
        ))
    for copy in final_sent:
        copy.start()
    final_rows[pl.ds(own_slot, 1)] = final_row[...][None]
    end_strip_sum()
    for i in range(1, devices * strips):
        t, z = lax.rem(me + i // strips, devices), lax.rem(strip + i % strips, strips)
        spot = final_rows.at[final_slot(t, z)]
        pltpu.make_async_remote_copy(
            src_ref=spot, dst_ref=spot, send_sem=fs_sem.at[i], recv_sem=fr_sem.at[final_slot(t, z)],
            device_id={"tm": t, "space": z}, device_id_type=DEVICE,
        ).wait_recv()
    total = final_rows[0]
    for i in range(1, devices * strips):
        total = total + final_rows[i]
    tile[LEVELS:LEVELS + 1, :] = total
    summed = jnp.sum(tile[...], axis=1, keepdims=True)
    norms_out[...] = jnp.broadcast_to(jnp.sqrt(summed * (1.0 / cells)), (TILE, LANES))

    @pl.when(jnp.logical_not(last))
    def _():
        for copy in guess_shift + early_shift:
            copy.wait_send()

    for copy in handed + swaps + back_own + final_sent:
        copy.wait_send()
    for i in range(3):
        @pl.when(has_before[i])
        def _():
            back_before[i].wait_send()

    @pl.when(inner_chip)
    def _():
        to_sibling.wait_send()

    @pl.when(core == 0)
    def _():
        for copy in relays:
            copy.wait_send()


def fast_body(rhs, guess, diffusion):
    devices, strips = lax.axis_size("tm"), lax.axis_size("space")
    rows, width = rhs.shape[1:]
    tiles = width // LANES
    cells = rows * strips * width

    def spread(height):
        return height + (TILE - height) % (4 * TILE)

    def plane(*lead):
        return pltpu.VMEM(lead + (tiles, spread(rows + 2 * EDGE), LANES), jnp.float32)

    def coarse(*lead):
        return pltpu.VMEM(lead + (tiles, spread(rows // devices + 2 * EDGE), LANES), jnp.float32)

    dma = pltpu.SemaphoreType.DMA
    scratch = [
        plane(2), plane(2), plane(), plane(2), plane(), plane(), plane(2),
        plane(), plane(), plane(), plane(), plane(), plane(2),
        coarse(LEVELS - 1), tuple(coarse(devices >> level) for level in range(LEVELS - 1)),
        tuple(coarse(devices >> level) for level in range(LEVELS - 2)), coarse(), coarse(devices),
        pltpu.VMEM((TILE, LANES), jnp.float32),
        pltpu.VMEM((devices, TILE, LANES), jnp.float32),
        pltpu.VMEM((strips, TILE, LANES), jnp.float32),
        pltpu.VMEM((1, LANES), jnp.float32),
        pltpu.VMEM((devices * strips, 1, LANES), jnp.float32),
        dma((5, tiles)), dma((7, 2)), dma((7, 2)), dma((3, 4)), dma((3, 4)), dma((devices,)), dma((devices,)), dma,
        dma((devices,)), dma((devices,)), dma((2, devices)), dma((2, devices)), dma((2,)), dma((devices,)),
        dma((devices,)), dma((devices,)), dma((strips,)), dma((strips,)),
        dma((devices * strips,)), dma((devices * strips,)),
    ]
    any_space = pl.BlockSpec(memory_space=pl.ANY)
    result, norms = pl.pallas_call(
        functools.partial(cycle_kernel, strips, devices, cells),
        out_shape=(
            pltpu.VMEM(rhs.shape, jnp.float32),
            jax.ShapeDtypeStruct((TILE, LANES), jnp.float32),
        ),
        in_specs=[any_space] * 3,
        out_specs=(pl.BlockSpec(memory_space=pltpu.VMEM), pl.BlockSpec(memory_space=pltpu.VMEM)),
        scratch_shapes=scratch,
        compiler_params=pltpu.CompilerParams(
            collective_id=0, has_side_effects=True, vmem_limit_bytes=67_043_328 - rhs.size * 4 - 2**17
        ),
    )(rhs, guess, diffusion)
    return result, norms[:LEVELS + 1, 0]


def solution(mesh):
    in_specs = (P("tm", "space", None), P("tm", "space", None), P("space", None))
    out_specs = (P("tm", "space", None), P())

    def choose(rhs, guess, diffusion):
        points = rhs.shape[0] * lax.axis_size("tm")
        one_coarsest = points == 2 ** (LEVELS - 1) and rhs.shape[0] == 2
        even = rhs.shape[1] % (TILE * lax.axis_size("tm")) == 0 and rhs.shape[2] % 128 == 0
        if one_coarsest and even:
            return fast_body(rhs, guess, diffusion)
        return body(rhs, guess, diffusion)

    return jax.shard_map(choose, mesh=mesh, in_specs=in_specs, out_specs=out_specs, check_vma=False)
```

```python
import functools

import jax
import jax.numpy as jnp
from jax import lax
from jax.experimental import pallas as pl
from jax.experimental.pallas import tpu as pltpu
from jax.sharding import PartitionSpec as P

LEVELS = 5


damping = 0.8


def with_halo(block, sides, width):
    for axis, dim in sides:
        count = lax.axis_size(axis)
        forward = [(i, i + 1) for i in range(count - 1)]
        backward = [(target, source) for source, target in forward]
        low = lax.ppermute(
            lax.slice_in_dim(block, block.shape[dim] - width, None, axis=dim), axis, forward
        )
        high = lax.ppermute(lax.slice_in_dim(block, 0, width, axis=dim), axis, backward)
        block = jnp.concatenate([low, block, high], axis=dim)
    return block


def shifted(value, axis, steps):
    count = lax.axis_size(axis)
    first, last = (max(0, -steps), min(count, count - steps))
    return lax.ppermute(value, axis, [(source, source + steps) for source in range(first, last)])


def from_partner(value, axis, apart):
    mask = 2**apart
    pairs = [(source, source ^ mask) for source in range(lax.axis_size(axis))]
    return lax.ppermute(value, axis, pairs)


def neighbours(field):
    rows = with_halo(field, (("space", 1),), 1)
    padded = jnp.pad(rows, ((0, 0), (0, 0), (1, 1)))
    total = padded[:, 2:, 1:-1] + padded[:, :-2, 1:-1]
    total = total + padded[:, 1:-1, 2:] + padded[:, 1:-1, :-2]
    return total


def residual(field, source, scaled, diag, stride):
    earlier = shifted(field[-1:], "tm", stride)
    before = jnp.concatenate([earlier, field[:-1]], axis=0)
    image = diag * field - scaled * neighbours(field) - before
    return source - image


def stride_of(level):
    if level == 0:
        return 1
    return 2 ** (level - 1)


def body(rhs, guess, diffusion):
    position = lax.axis_index("tm")
    cells = rhs.shape[1] * lax.axis_size("space") * rhs.shape[2]
    partials = []

    def weight_of(level):
        if level <= 1:
            return jnp.float32(1.0)
        stride = stride_of(level)
        return jnp.where(position % stride == stride - 1, 1.0, 0.0).astype(jnp.float32)

    def record(resid, level):
        local_part = jnp.sum(resid * resid) * weight_of(level)
        partials.append(local_part)

    sources = [rhs]
    fields = []
    field = guess
    for level in range(LEVELS - 1):
        source = sources[level]
        scaled = 2.0**level * diffusion
        diag = 1.0 + 4.0 * scaled
        stride = stride_of(level)
        if level == 0:
            field = field + damping * residual(field, source, scaled, diag, stride) / diag
        else:
            field = damping * source / diag
        resid = residual(field, source, scaled, diag, stride)
        record(resid, level)
        fields.append(field)
        if level == 0:
            coarse = resid[0:1] + resid[1:2]
        else:
            coarse = resid + from_partner(resid, "tm", level - 1)
        sources.append(coarse)
    level = LEVELS - 1
    source = sources[level]
    scaled = 2.0**level * diffusion
    diag = 1.0 + 4.0 * scaled
    stride = stride_of(level)
    field = damping * source / diag
    field = field + damping * residual(field, source, scaled, diag, stride) / diag
    resid = residual(field, source, scaled, diag, stride)
    record(resid, level)
    correction = field
    for level in range(LEVELS - 2, -1, -1):
        scaled = 2.0**level * diffusion
        diag = 1.0 + 4.0 * scaled
        stride = stride_of(level)
        field = fields[level] + correction
        field = field + damping * residual(field, sources[level], scaled, diag, stride) / diag
        correction = field
    scaled = 1.0 * diffusion
    diag = 1.0 + 4.0 * scaled
    resid = residual(correction, rhs, scaled, diag, 1)
    record(resid, 0)
    totals = lax.psum(jnp.stack(partials), ("tm", "space"))
    norms = jnp.sqrt(totals / cells)
    return (correction, norms)


DEVICE = pl.DeviceIdType.MESH
TILE = 8
EDGE = 2 * TILE
BLOCK = 64
EARLY = 5
LANES = 128


def cycle_kernel(
    strips, devices, cells,
    rhs_in, guess_in, diff_in, out, norms_out,
    rhs, guess, diff, v0, v1, v1f, sol, guess_e, v0_e, v1f_e, early, early_e, weights,
    c_weights, c_fields, c_sums, c_top, c_v1f, tile, gathered, gathered_z, final_row, final_rows,
    load_sem, zs_sem, zr_sem, ts_sem, tr_sem, as_sem, ar_sem, al_sem,
    hs_sem, hr_sem, bs_sem, br_sem, bl_sem, rs_sem, ns_sem, nr_sem, ms_sem, mr_sem, fs_sem, fr_sem,
):
    me = lax.axis_index("tm")
    strip = lax.axis_index("space")
    rows, width = rhs_in.shape[1], rhs_in.shape[2]
    tiles = width // LANES
    core = lax.rem(me, 2)
    sibling = me + 1 - 2 * core
    chip = me // 2
    chip_x = chip + 1 - 2 * lax.rem(chip, 2)
    chip_y = lax.rem(chip + 2, 4)
    chip_xy = lax.rem(chip_x + 2, 4)
    low, high = EDGE, EDGE + rows
    first, last = me == 0, me == devices - 1
    top, bottom = strip == 0, strip == strips - 1
    piece = rows // devices
    tall_piece = piece + 2 * TILE

    def aligned(value):
        return pl.multiple_of(value, TILE)

    def tm_copy(src, dst, send, recv, target):
        return pltpu.make_async_remote_copy(
            src_ref=src, dst_ref=dst, send_sem=send, recv_sem=recv,
            device_id={"tm": target, "space": strip}, device_id_type=DEVICE,
        )

    def space_copy(src, dst, send, recv, target):
        return pltpu.make_async_remote_copy(
            src_ref=src, dst_ref=dst, send_sem=send, recv_sem=recv,
            device_id={"tm": me, "space": target}, device_id_type=DEVICE,
        )

    later = jnp.minimum(me + 1, devices - 1)
    inside = slice(low, high)

    def load(index, source, target):
        return [
            pltpu.make_async_copy(
                source.at[:, j * LANES:(j + 1) * LANES], target.at[j, inside], load_sem.at[index, j]
            )
            for j in range(tiles)
        ]

    loads = [
        load(0, guess_in.at[1], guess.at[1]), load(1, guess_in.at[0], guess.at[0]), load(2, diff_in, diff),
        load(3, rhs_in.at[1], rhs.at[1]), load(4, rhs_in.at[0], rhs.at[0]),
    ]
    for group in loads:
        for copy in group:
            copy.start()

    barrier = pltpu.get_barrier_semaphore()
    for i in range(1, devices):
        pl.semaphore_signal(
            barrier, inc=1, device_id={"tm": lax.rem(me + i, devices), "space": strip}, device_id_type=DEVICE
        )
    down = jnp.minimum(strip + 1, strips - 1)
    up = jnp.maximum(strip - 1, 0)
    for edge, beside in ((top, up), (bottom, down)):
        @pl.when(jnp.logical_not(edge))
        def _():
            pl.semaphore_signal(barrier, inc=1, device_id={"tm": me, "space": beside}, device_id_type=DEVICE)

    def row_tiles(start, size):
        return [start + i * TILE for i in range(size // TILE)]

    def blocks(start, size, step, carry=0):
        count = size // BLOCK

        def run(i, carry):
            begin = aligned(start + i * BLOCK)
            for offset in range(0, BLOCK, TILE):
                carry = step(begin + offset, carry)
            return carry

        if count == 1:
            carry = run(0, carry)
        elif count:
            carry = lax.fori_loop(0, count, run, carry)
        for r in row_tiles(start + count * BLOCK, size - count * BLOCK):
            carry = step(r, carry)
        return carry

    def at(r):
        return pl.ds(r, TILE)

    zero = jnp.zeros((TILE, LANES), jnp.float32)

    @pl.when(first)
    def _():
        def clear(r, carry):
            for ref in (guess_e, v0_e, v1f_e, early_e):
                for j in range(tiles):
                    ref[j, at(r), :] = zero
            return carry

        blocks(low - TILE, rows + 2 * TILE, clear)

    def clear_edge(start):
        for j in range(tiles):
            for ref in (guess, rhs):
                for p in range(2):
                    ref[p, j, start:start + TILE, :] = zero
            for ref in (v1, v1f, guess_e, v0_e, diff):
                ref[j, start:start + TILE, :] = zero

    @pl.when(top)
    def _():
        clear_edge(low - TILE)

    @pl.when(bottom)
    def _():
        clear_edge(high)

    pl.semaphore_wait(barrier, devices + 1 - top.astype(jnp.int32) - bottom.astype(jnp.int32))

    def halo_pair(index, field, lead=()):
        def rows_at(start):
            return field.at[lead + (slice(None), slice(start, start + TILE))]

        return (
            space_copy(rows_at(high - TILE), rows_at(low - TILE), zs_sem.at[index, 0], zr_sem.at[index, 0], down),
            space_copy(rows_at(low), rows_at(high), zs_sem.at[index, 1], zr_sem.at[index, 1], up),
        )

    guess_halo = halo_pair(0, guess, (slice(None),))
    diff_halo = halo_pair(1, diff)
    rhs_halo = halo_pair(2, rhs, (slice(None),))
    v1_halo, v1f_halo, guess_e_halo, v0_e_halo = [
        halo_pair(3 + i, field) for i, field in enumerate((v1, v1f, guess_e, v0_e))
    ]

    def start_halo(pair_of):
        @pl.when(jnp.logical_not(bottom))
        def _():
            pair_of[0].start()

        @pl.when(jnp.logical_not(top))
        def _():
            pair_of[1].start()

    def finish_halo(pair_of):
        @pl.when(jnp.logical_not(top))
        def _():
            pair_of[0].wait_recv()
            pair_of[1].wait_send()

        @pl.when(jnp.logical_not(bottom))
        def _():
            pair_of[1].wait_recv()
            pair_of[0].wait_send()

    half = rows // 2
    quarter = rows // 4
    whole = [
        (low - TILE, quarter + TILE), (low + quarter, quarter),
        (low + 2 * quarter, quarter), (low + 3 * quarter, quarter + TILE),
    ]
    inner = [(low + quarter * j, quarter) for j in range(4)]
    guess_parts = [(low, half), (low + half, half)]

    def shift(stage, source, target, parts):
        return [
            tm_copy(
                source.at[:, start:start + size], target.at[:, start:start + size],
                ts_sem.at[stage, j], tr_sem.at[stage, j], later,
            )
            for j, (start, size) in enumerate(parts)
        ]

    def send(copy):
        @pl.when(jnp.logical_not(last))
        def _():
            copy.start()

    def receive(copy):
        @pl.when(jnp.logical_not(first))
        def _():
            copy.wait_recv()

    guess_shift = shift(0, guess.at[1], guess_e, guess_parts)
    v0_shift = shift(1, v0.at[1], v0_e, inner)
    early_parts = [(low + rows // 8 * j, rows // 8) for j in range(8)]
    early_shift = shift(2, early, early_e, early_parts)

    for copy in loads[0]:
        copy.wait()
    send(guess_shift[0])
    send(guess_shift[1])
    for copy in loads[1]:
        copy.wait()
    start_halo(guess_halo)
    for copy in loads[2]:
        copy.wait()
    start_halo(diff_halo)
    for copy in loads[3] + loads[4]:
        copy.wait()
    start_halo(rhs_halo)

    lane = lax.broadcasted_iota(jnp.int32, (TILE, LANES), 1)
    at_left, at_right = lane == 0, lane == LANES - 1

    def stencil(field, r):
        mids = [field[j, at(r), :] for j in range(tiles)]
        right = [zero] + [pltpu.roll(mid, 1, 1) for mid in mids]
        left = [pltpu.roll(mid, LANES - 1, 1) for mid in mids] + [zero]
        totals = []
        for j in range(tiles):
            total = field[j, at(r - 1), :] + field[j, at(r + 1), :]
            total = total + jnp.where(at_left, right[j], right[j + 1])
            totals.append(total + jnp.where(at_right, left[j + 1], left[j]))
        return mids, totals

    def squares(values):
        total = values[0] * values[0]
        for value in values[1:]:
            total = total + value * value
        return total

    keep_share = 1.0 - damping

    def set_weights(r, carry):
        for j in range(tiles):
            scaled = diff[j, at(r), :]
            for level in range(2):
                weights[level, j, at(r), :] = damping / (1.0 + 4.0 * (2.0**level * scaled))
        return carry

    def sweep(p, source, before, target, also=None):
        def step(r, carry):
            mids, totals = stencil(source, r)
            for j in range(tiles):
                inner_sum = rhs[p, j, at(r), :] + diff[j, at(r), :] * totals[j] + before[j, at(r), :]
                value = keep_share * mids[j] + weights[0, j, at(r), :] * inner_sum
                target[j, at(r), :] = value
                if also is not None:
                    also(j, r, value)
            return carry

        return step

    def level_residual(p, j, r, mid, total, before):
        scaled = diff[j, at(r), :]
        return rhs[p, j, at(r), :] - mid + scaled * (total - 4.0 * mid) + before

    sweep_last = sweep(1, guess.at[1], guess.at[0], v0.at[1])
    blocks(low, rows, set_weights)
    blocks(low + quarter, 2 * quarter, sweep_last)
    finish_halo(guess_halo)
    finish_halo(diff_halo)
    finish_halo(rhs_halo)
    set_weights(low - TILE, 0)
    set_weights(high, 0)
    for j in (0, 3):
        blocks(*whole[j], sweep_last)
    for j in (0, 3, 1, 2):
        send(v0_shift[j])

    c_low, c_high = EDGE, EDGE + piece
    c_rows = slice(c_low - TILE, c_high + TILE)
    c_tiles, c_own = row_tiles(c_low - TILE, tall_piece), row_tiles(c_low, piece)
    offset = me * piece

    def coarse_diff(j, r):
        return diff[j, at(aligned(r + offset)), :]

    def coarse_weights(i, carry):
        r = aligned(c_low - TILE + i * TILE)
        for j in range(tiles):
            base = coarse_diff(j, r)
            for level in range(1, LEVELS):
                c_weights[level - 1, j, at(r), :] = damping / (1.0 + 4.0 * (2.0**level * base))
        return carry

    lax.fori_loop(0, tall_piece // TILE, coarse_weights, 0)

    def keep_early(j, r, value):
        early[j, at(r), :] = rhs[1, j, at(r), :] + value

    for copy in guess_shift:
        receive(copy)

    @pl.when(jnp.logical_not(first))
    def _():
        start_halo(guess_e_halo)

    halo_tiles = (low - TILE, high)
    sweep_first = sweep(0, guess.at[0], guess_e, v0.at[0], keep_early)
    blocks(low, rows, sweep_first)

    @pl.when(jnp.logical_not(first))
    def _():
        finish_halo(guess_e_halo)

    for r in halo_tiles:
        sweep_first(r, 0)

    def descend(r, carry):
        firsts, totals = stencil(v0.at[0], r)
        lasts, totals_last = stencil(v0.at[1], r)
        ones, twos = [], []
        for j in range(tiles):
            ones.append(level_residual(0, j, r, firsts[j], totals[j], v0_e[j, at(r), :]))
            twos.append(level_residual(1, j, r, lasts[j], totals_last[j], firsts[j]))
            v1[j, at(r), :] = weights[1, j, at(r), :] * (ones[j] + twos[j])
        return carry + (squares(ones) + squares(twos))

    c_v1 = c_fields[0]

    def row_place(k, ahead=0):
        return aligned(low - ahead + k * piece)

    def hand_over(slot, k, side):
        ahead, size = TILE * (1 - side), piece + TILE
        return tm_copy(
            v1.at[:, pl.ds(row_place(k, ahead), size)],
            c_v1.at[me, :, pl.ds(aligned(c_low - ahead), size)],
            as_sem.at[slot], ar_sem.at[me], k,
        )

    total0 = zero
    for j in (0, 3, 1, 2):
        receive(v0_shift[j])
        total0 = blocks(*inner[j], descend, total0)
        if j == 3:
            start_halo(v1_halo)
    finish_halo(v1_halo)
    others = [2 * c + i for c in (chip_x, chip_y) for i in range(2)] + [sibling] + [2 * chip_xy, 2 * chip_xy + 1]
    far = others[:4] + others[5:]
    tall_here = v1.at[:, pl.ds(row_place(me, TILE), tall_piece)]
    tall_there = v1.at[:, pl.ds(row_place(sibling, TILE), tall_piece)]
    handed = [hand_over(slot, k, slot % 2) for slot, k in enumerate(far)]
    handed.insert(4, tm_copy(tall_there, c_v1.at[me, :, c_rows], as_sem.at[6], ar_sem.at[me], sibling))
    for copy in handed:
        copy.start()
    local = pltpu.make_async_copy(tall_here, c_v1.at[me, :, c_rows], al_sem)
    local.start()
    local.wait()
    for copy in early_shift[:EARLY]:
        send(copy)
    mine = pl.ds(aligned(c_low - TILE * (1 - core)), piece + TILE)
    inner_edge = pl.ds(aligned(c_low + (1 - core) * (piece - TILE)), TILE)
    outer_edge = pl.ds(aligned(c_low - TILE + core * (piece + TILE)), TILE)
    swaps = [
        tm_copy(c_v1.at[k, :, inner_edge], c_v1.at[k, :, outer_edge], hs_sem.at[slot], hr_sem.at[k], sibling)
        for slot, k in enumerate(far)
    ]
    for swap, k in zip(swaps, far):
        spot = c_v1.at[k, :, mine]
        tm_copy(spot, spot, hs_sem.at[0], ar_sem.at[k], sibling).wait_recv()
        swap.start()
    spot = c_v1.at[sibling, :, c_rows]
    tm_copy(spot, spot, hs_sem.at[0], ar_sem.at[sibling], sibling).wait_recv()
    for swap in swaps:
        swap.wait_recv()

    coarsest = LEVELS - 1

    def coarse_residual(level):
        field, target = c_fields[level - 1], c_fields[level]
        count = devices >> (level - 1)
        carry = zero
        for r in c_tiles:
            own = c_low <= r < c_high
            scaled = [2.0**level * coarse_diff(j, r) for j in range(tiles)]
            earlier, even = None, None
            for p in range(count):
                mids, totals = stencil(field.at[p], r)
                resid = []
                for j in range(tiles):
                    value = 0.25 * mids[j] + scaled[j] * (mids[j] + totals[j])
                    resid.append(value + earlier[j] if p else value)
                earlier = mids
                if own:
                    carry = carry + squares(resid)
                if p % 2 == 0:
                    even = resid
                else:
                    for j in range(tiles):
                        target[p // 2, j, at(r), :] = c_weights[level, j, at(r), :] * (even[j] + resid[j])
        return carry

    def lift(level, p, j, r, value):
        for q in (2 * p, 2 * p + 1):
            c_sums[level - 1][q, j, at(r), :] = c_fields[level - 1][q, j, at(r), :] + value

    def coarse_final(level, p, r, mids, totals, scaled, earlier):
        values = []
        for j in range(tiles):
            value = scaled[j] * totals[j]
            if p:
                value = value + earlier[j]
            value = c_fields[level - 1][p, j, at(r), :] + c_weights[level - 1, j, at(r), :] * value
            values.append(keep_share * mids[j] + value)
        return values

    parts = [total0]
    for level in range(1, coarsest):
        parts.append(coarse_residual(level))

    field_l = c_fields[coarsest - 1].at[0]
    for r in c_tiles:
        mids, totals = stencil(field_l, r)
        for j in range(tiles):
            scaled = 2.0**coarsest * coarse_diff(j, r)
            value = (1.0 + keep_share) * mids[j] + c_weights[coarsest - 1, j, at(r), :] * (scaled * totals[j])
            c_top[j, at(r), :] = value
            lift(coarsest - 1, 0, j, r, value)
    for level in range(coarsest - 1, 1, -1):
        for r in c_tiles:
            scaled = [2.0**level * coarse_diff(j, r) for j in range(tiles)]
            earlier = None
            for p in range(devices >> (level - 1)):
                mids, totals = stencil(c_sums[level - 1].at[p], r)
                values = coarse_final(level, p, r, mids, totals, scaled, earlier)
                earlier = mids
                for j in range(tiles):
                    lift(level - 1, p, j, r, values[j])

    total_l = zero
    for r in c_own:
        mids, totals = stencil(c_top, r)
        resid = []
        for j in range(tiles):
            scaled = 2.0**coarsest * coarse_diff(j, r)
            ahead = (1.0 + keep_share / damping) * field_l[j, at(r), :] - mids[j]
            resid.append((1.0 + 4.0 * scaled) * ahead + scaled * totals[j])
        total_l = total_l + squares(resid)
    parts.append(total_l)
    tile[...] = jnp.zeros((TILE, LANES), jnp.float32)
    for level, value in enumerate(parts):
        tile[level:level + 1, :] = jnp.sum(value, axis=0, keepdims=True)

    def begin_sum(count, own, slots, copier, send_sems, recv_sems):
        slots[pl.ds(own, 1)] = tile[...][None]
        sent = [
            copier(tile, slots.at[own], send_sems.at[i], recv_sems.at[own], lax.rem(own + i, count))
            for i in range(1, count)
        ]
        for copy in sent:
            copy.start()

        def end_sum():
            for i in range(1, count):
                other = lax.rem(own + i, count)
                copier(tile, slots.at[other], send_sems.at[i], recv_sems.at[other], other).wait_recv()
            for copy in sent:
                copy.wait_send()
            total = slots[0]
            for i in range(1, count):
                total = total + slots[i]
            tile[...] = total

        return end_sum

    end_time_sum = begin_sum(devices, me, gathered, tm_copy, ns_sem, nr_sem)

    place = pl.ds(row_place(me), piece)

    def give_back(kind, slot, target, point):
        src, dst = c_v1f.at[point, :, c_low:c_high], (v1f, v1f_e)[kind].at[:, place]
        return tm_copy(src, dst, bs_sem.at[kind, slot], br_sem.at[kind, me], target)

    def keep_back(kind, point):
        src, dst = c_v1f.at[point, :, c_low:c_high], (v1f, v1f_e)[kind].at[:, place]
        local = pltpu.make_async_copy(src, dst, bl_sem.at[kind])
        local.start()
        local.wait()

    for r in c_own:
        scaled = [2.0 * coarse_diff(j, r) for j in range(tiles)]
        earlier = None
        for p in range(devices):
            mids, totals = stencil(c_sums[0].at[p], r)
            values = coarse_final(1, p, r, mids, totals, scaled, earlier)
            earlier = mids
            for j in range(tiles):
                c_v1f[p, j, at(r), :] = values[j]
    back_own = [give_back(0, slot, k, k) for slot, k in enumerate(others)]
    back_before = [give_back(1, slot, 2 * c, jnp.maximum(2 * c - 1, 0)) for slot, c in enumerate((chip_x, chip_y, chip_xy))]
    to_sibling = give_back(1, 3, sibling, jnp.maximum(sibling - 1, 0))
    has_before = [c > 0 for c in (chip_x, chip_y, chip_xy)]
    inner_chip = jnp.logical_and(core == 1, chip > 0)

    def start_before(i):
        @pl.when(has_before[i])
        def _():
            back_before[i].start()

    for copy in back_own[:4]:
        copy.start()
    start_before(0)
    start_before(1)
    for copy in back_own[5:]:
        copy.start()
    start_before(2)
    back_own[4].start()

    @pl.when(inner_chip)
    def _():
        to_sibling.start()

    keep_back(0, me)

    @pl.when(jnp.logical_and(core == 0, chip > 0))
    def _():
        keep_back(1, jnp.maximum(me - 1, 0))

    for copy in early_shift[EARLY:]:
        send(copy)

    @pl.when(jnp.logical_not(last))
    def _():
        for copy in v0_shift:
            copy.wait_send()

    def spots_of(field, k):
        return field.at[:, pl.ds(row_place(k), piece)]

    def relay(slot, k):
        return tm_copy(spots_of(v1f, k), spots_of(v1f_e, k), rs_sem.at[slot], br_sem.at[1, k], sibling)

    def absorb(spots):
        for r in spots:
            for j in range(tiles):
                value = v1f[j, at(r), :]
                for p in range(2):
                    v0[p, j, at(r), :] = v0[p, j, at(r), :] + value

    order = [me, sibling] + others[:4] + others[5:]
    relays = [relay(slot, k) for slot, k in enumerate(order)]

    def place_tiles(k):
        return [row_place(k) + i * TILE for i in range(piece // TILE)]

    for slot, k in enumerate(order):
        if slot:
            spots = spots_of(v1f, k)
            tm_copy(spots, spots, rs_sem.at[slot], br_sem.at[0, k], sibling).wait_recv()

        @pl.when(core == 0)
        def _():
            relays[slot].start()

        absorb(place_tiles(k))
    start_halo(v1f_halo)
    def ascend_last(r, carry, store=True):
        mids, totals = stencil(v0.at[1], r)
        for j in range(tiles):
            inner_sum = rhs[1, j, at(r), :] + diff[j, at(r), :] * totals[j] + v0[0, j, at(r), :]
            value = keep_share * mids[j] + weights[0, j, at(r), :] * inner_sum
            sol[1, j, at(r), :] = value
            if store:
                out[1, at(r - low), j * LANES:(j + 1) * LANES] = value
        return carry

    def ascend_first(r, carry):
        mids, totals = stencil(v0.at[0], r)
        for j in range(tiles):
            inner_sum = rhs[0, j, at(r), :] + diff[j, at(r), :] * totals[j]
            sol[0, j, at(r), :] = keep_share * mids[j] + weights[0, j, at(r), :] * inner_sum
        return carry

    def ascend_inside(r, carry):
        return ascend_first(r, ascend_last(r, carry))

    blocks(low + TILE, rows - 2 * TILE, ascend_inside)
    finish_halo(v1f_halo)
    absorb(halo_tiles)
    for r in (low, high - TILE):
        ascend_inside(r, 0)
    for r in halo_tiles:
        ascend_last(r, 0, False)
        ascend_first(r, 0)

    def final_last(r, carry):
        mids, totals = stencil(sol.at[1], r)
        for j in range(tiles):
            rhs[1, j, at(r), :] = level_residual(1, j, r, mids[j], totals[j], 0.0)
        return carry

    blocks(low, rows, final_last)
    end_time_sum()
    end_strip_sum = begin_sum(strips, strip, gathered_z, space_copy, ms_sem, mr_sem)

    def complete(r, carry):
        resid = []
        for j in range(tiles):
            before = v0_e[j, at(r), :] + v1f_e[j, at(r), :]
            v0_e[j, at(r), :] = before
            value = sol[0, j, at(r), :] + weights[0, j, at(r), :] * before
            sol[0, j, at(r), :] = value
            out[0, at(r - low), j * LANES:(j + 1) * LANES] = value
            resid.append(rhs[1, j, at(r), :] + value)
        return carry + squares(resid)

    total5 = zero
    for slot, k in enumerate(order):
        @pl.when(jnp.logical_or(core == 1, chip > 0) if slot else core == 1)
        def _():
            relays[slot].wait_recv()

        for r in place_tiles(k):
            total5 = complete(r, total5)

    @pl.when(jnp.logical_not(first))
    def _():
        start_halo(v0_e_halo)

    def final_first(r, carry):
        mids, totals = stencil(v0_e, r)
        befores = []
        for j in range(tiles):
            inner_sum = early_e[j, at(r), :] + v1f_e[j, at(r), :] + diff[j, at(r), :] * totals[j]
            befores.append(keep_share * mids[j] + weights[0, j, at(r), :] * inner_sum)
        mids, totals = stencil(sol.at[0], r)
        return carry + squares([
            level_residual(0, j, r, mids[j], totals[j], befores[j]) for j in range(tiles)
        ])

    for i, copy in enumerate(early_shift):
        receive(copy)
        begin, size = early_parts[i]
        cut_low, cut_high = TILE * (i == 0), TILE * (i == len(early_parts) - 1)
        total5 = blocks(begin + cut_low, size - cut_low - cut_high, final_first, total5)

    @pl.when(jnp.logical_not(first))
    def _():
        finish_halo(v0_e_halo)

    for r in halo_tiles:
        for j in range(tiles):
            sol[0, j, at(r), :] = sol[0, j, at(r), :] + weights[0, j, at(r), :] * v0_e[j, at(r), :]
    for r in (low, high - TILE):
        total5 = final_first(r, total5)

    final_row[...] = jnp.sum(total5, axis=0, keepdims=True)

    def final_slot(t, z):
        return t * strips + z

    own_slot = final_slot(me, strip)
    final_sent = []
    for i in range(1, devices * strips):
        t, z = lax.rem(me + i // strips, devices), lax.rem(strip + i % strips, strips)
        final_sent.append(pltpu.make_async_remote_copy(
            src_ref=final_row, dst_ref=final_rows.at[own_slot], send_sem=fs_sem.at[i], recv_sem=fr_sem.at[own_slot],
            device_id={"tm": t, "space": z}, device_id_type=DEVICE,
        ))
    for copy in final_sent:
        copy.start()
    final_rows[pl.ds(own_slot, 1)] = final_row[...][None]
    end_strip_sum()
    for i in range(1, devices * strips):
        t, z = lax.rem(me + i // strips, devices), lax.rem(strip + i % strips, strips)
        spot = final_rows.at[final_slot(t, z)]
        pltpu.make_async_remote_copy(
            src_ref=spot, dst_ref=spot, send_sem=fs_sem.at[i], recv_sem=fr_sem.at[final_slot(t, z)],
            device_id={"tm": t, "space": z}, device_id_type=DEVICE,
        ).wait_recv()
    total = final_rows[0]
    for i in range(1, devices * strips):
        total = total + final_rows[i]
    tile[LEVELS:LEVELS + 1, :] = total
    summed = jnp.sum(tile[...], axis=1, keepdims=True)
    roots = jnp.sqrt(summed * (1.0 / cells))
    for level in range(LEVELS + 1):
        norms_out[level] = roots[level, 0]

    @pl.when(jnp.logical_not(last))
    def _():
        for copy in guess_shift + early_shift:
            copy.wait_send()

    for copy in handed + swaps + back_own + final_sent:
        copy.wait_send()
    for i in range(3):
        @pl.when(has_before[i])
        def _():
            back_before[i].wait_send()

    @pl.when(inner_chip)
    def _():
        to_sibling.wait_send()

    @pl.when(core == 0)
    def _():
        for copy in relays:
            copy.wait_send()


def fast_body(rhs, guess, diffusion):
    devices, strips = lax.axis_size("tm"), lax.axis_size("space")
    rows, width = rhs.shape[1:]
    tiles = width // LANES
    cells = rows * strips * width

    def spread(height):
        return height + (TILE - height) % (4 * TILE)

    def plane(*lead):
        return pltpu.VMEM(lead + (tiles, spread(rows + 2 * EDGE), LANES), jnp.float32)

    def coarse(*lead):
        return pltpu.VMEM(lead + (tiles, spread(rows // devices + 2 * EDGE), LANES), jnp.float32)

    dma = pltpu.SemaphoreType.DMA
    scratch = [
        plane(2), plane(2), plane(), plane(2), plane(), plane(), plane(2),
        plane(), plane(), plane(), plane(), plane(), plane(2),
        coarse(LEVELS - 1), tuple(coarse(devices >> level) for level in range(LEVELS - 1)),
        tuple(coarse(devices >> level) for level in range(LEVELS - 2)), coarse(), coarse(devices),
        pltpu.VMEM((TILE, LANES), jnp.float32),
        pltpu.VMEM((devices, TILE, LANES), jnp.float32),
        pltpu.VMEM((strips, TILE, LANES), jnp.float32),
        pltpu.VMEM((1, LANES), jnp.float32),
        pltpu.VMEM((devices * strips, 1, LANES), jnp.float32),
        dma((5, tiles)), dma((7, 2)), dma((7, 2)), dma((3, 8)), dma((3, 8)), dma((devices,)), dma((devices,)), dma,
        dma((devices,)), dma((devices,)), dma((2, devices)), dma((2, devices)), dma((2,)), dma((devices,)),
        dma((devices,)), dma((devices,)), dma((strips,)), dma((strips,)),
        dma((devices * strips,)), dma((devices * strips,)),
    ]
    any_space = pl.BlockSpec(memory_space=pl.ANY)
    result, norms = pl.pallas_call(
        functools.partial(cycle_kernel, strips, devices, cells),
        out_shape=(
            pltpu.VMEM(rhs.shape, jnp.float32),
            jax.ShapeDtypeStruct((LEVELS + 1,), jnp.float32),
        ),
        in_specs=[any_space] * 3,
        out_specs=(pl.BlockSpec(memory_space=pltpu.VMEM), pl.BlockSpec(memory_space=pltpu.SMEM)),
        scratch_shapes=scratch,
        compiler_params=pltpu.CompilerParams(
            collective_id=0, has_side_effects=True, vmem_limit_bytes=67_043_328 - rhs.size * 4 - 2**17
        ),
    )(rhs, guess, diffusion)
    return result, norms


def solution(mesh):
    in_specs = (P("tm", "space", None), P("tm", "space", None), P("space", None))
    out_specs = (P("tm", "space", None), P())

    def choose(rhs, guess, diffusion):
        points = rhs.shape[0] * lax.axis_size("tm")
        one_coarsest = points == 2 ** (LEVELS - 1) and rhs.shape[0] == 2
        even = rhs.shape[1] % (TILE * lax.axis_size("tm")) == 0 and rhs.shape[2] % 128 == 0
        if one_coarsest and even:
            return fast_body(rhs, guess, diffusion)
        return body(rhs, guess, diffusion)

    return jax.shard_map(choose, mesh=mesh, in_specs=in_specs, out_specs=out_specs, check_vma=False)
```
